8 devices in a mesh: replica: 4 (over z, y, x), data: 2 (over core).
Axes of the slice: x: 2, y: 2, z: 1, core: 2. Of those that a mesh axis runs over, the one named last changes fastest.
Arguments:
- inp_rows: bfloat16 [32768, 768], P(('replica', 'data'))
- out_grad: bfloat16 [32768, 768], P(('replica', 'data'))
- w_up: bfloat16 [2, 768, 3072], replicated
- w_down: bfloat16 [2, 3072, 768], replicated
- master_up: float32 [2, 768, 3072], P(None, 'data')
- master_down: float32 [2, 3072, 768], P(None, 'data')
- mom_up: float32 [2, 768, 3072], P(None, 'data')
- mom_down: float32 [2, 3072, 768], P(None, 'data')
- var_up: float32 [2, 768, 3072], P(None, 'data')
- var_down: float32 [2, 3072, 768], P(None, 'data')
- clip_norm: float32 [], replicated
Outputs:
- output 1: bfloat16 [2, 768, 3072], replicated
- output 2: bfloat16 [2, 3072, 768], replicated
- output 3: float32 [2, 768, 3072], P(None, 'data')
- output 4: float32 [2, 3072, 768], P(None, 'data')
- output 5: float32 [2, 768, 3072], P(None, 'data')
- output 6: float32 [2, 3072, 768], P(None, 'data')
- output 7: float32 [2, 768, 3072], P(None, 'data')
- output 8: float32 [2, 3072, 768], P(None, 'data')
- output 9: float32 [], replicated
All inputs are finite; a program needn't handle non-finite values.
Results may differ from the reference program's by a relative error of at most 0.0110299.
Values are sent between devices in bfloat16 or wider.
A program may use at most 1 GiB of HBM per device.

```python
import jax
import jax.numpy as jnp
from jax import lax

D = 768
FF = 3072
B_LOCAL = 4096
REPLICA = 4
DATA = 2
STEP = 10
DEVICES = REPLICA * DATA
ROWS = B_LOCAL * DEVICES
BETA1 = 0.9
BETA2 = 0.95
ADAM_EPS = 1e-8
LEARN_RATE = 5e-3
NORM_EPS = 1e-6
BIAS_ONE = 1.0 - BETA1 ** STEP
BIAS_TWO = 1.0 - BETA2 ** STEP


def gelu_value(pre_act):
    return pre_act * (0.5 + 0.5 * lax.erf(pre_act * 0.7071067811865476))


def gelu_slope(pre_act):
    return 0.5 + 0.5 * lax.erf(pre_act * 0.7071067811865476) + pre_act * jnp.exp(-0.5 * pre_act * pre_act) * 0.3989422804014327


def matmul(left_mat, right_mat):
    return jnp.dot(left_mat, right_mat, preferred_element_type=jnp.float32)


def device_grads(inp_rows, out_grad, w_up, w_down):
    pre_one = matmul(inp_rows, w_up[0]).astype(jnp.bfloat16)
    act_one = gelu_value(pre_one.astype(jnp.float32)).astype(jnp.bfloat16)
    mid_rows = matmul(act_one, w_down[0]).astype(jnp.bfloat16)
    pre_two = matmul(mid_rows, w_up[1]).astype(jnp.bfloat16)
    act_two = gelu_value(pre_two.astype(jnp.float32)).astype(jnp.bfloat16)
    grad_down2 = matmul(act_two.T, out_grad)
    dact_two = matmul(out_grad, w_down[1].T).astype(jnp.bfloat16)
    dpre_two = (dact_two.astype(jnp.float32) * gelu_slope(pre_two.astype(jnp.float32))).astype(jnp.bfloat16)
    grad_up2 = matmul(mid_rows.T, dpre_two)
    dmid_rows = matmul(dpre_two, w_up[1].T).astype(jnp.bfloat16)
    grad_down1 = matmul(act_one.T, dmid_rows)
    dact_one = matmul(dmid_rows, w_down[0].T).astype(jnp.bfloat16)
    dpre_one = (dact_one.astype(jnp.float32) * gelu_slope(pre_one.astype(jnp.float32))).astype(jnp.bfloat16)
    grad_up1 = matmul(inp_rows.T, dpre_one)
    return jnp.stack([grad_up1, grad_up2]), jnp.stack([grad_down1, grad_down2])


def mean_grads(inp_rows, out_grad, w_up, w_down):
    inp_blocks = inp_rows.reshape(DEVICES, B_LOCAL, D)
    grad_blocks = out_grad.reshape(DEVICES, B_LOCAL, D)

    def scan_step(carry_sums, block_pair):
        up_part, down_part = device_grads(block_pair[0], block_pair[1], w_up, w_down)
        return (carry_sums[0] + up_part, carry_sums[1] + down_part), None

    zero_carry = (jnp.zeros((2, D, FF), jnp.float32), jnp.zeros((2, FF, D), jnp.float32))
    totals, unused = lax.scan(scan_step, zero_carry, (inp_blocks, grad_blocks))
    return totals[0] / DEVICES, totals[1] / DEVICES


def adam_update(grad_vals, master_vals, mom_vals, var_vals, clip_scale):
    new_mom = BETA1 * mom_vals + (1.0 - BETA1) * clip_scale * grad_vals
    new_var = BETA2 * var_vals + (1.0 - BETA2) * (clip_scale * clip_scale) * (grad_vals * grad_vals)
    new_master = master_vals - LEARN_RATE * (new_mom / BIAS_ONE) / (jnp.sqrt(new_var / BIAS_TWO) + ADAM_EPS)
    return new_master, new_mom, new_var


def setup_inputs(seed: int = 0) -> dict:
    keys = jax.random.split(jax.random.key(seed), 9)
    inp_rows = jax.random.normal(keys[0], (ROWS, D), jnp.float32).astype(jnp.bfloat16)
    out_grad = jax.random.normal(keys[1], (ROWS, D), jnp.float32).astype(jnp.bfloat16)
    down_gain = jnp.array([1.6, 1.4], jnp.float32).reshape(2, 1, 1)
    master_up = jax.random.normal(keys[2], (2, D, FF), jnp.float32) * D ** -0.5
    master_down = jax.random.normal(keys[3], (2, FF, D), jnp.float32) * down_gain * FF ** -0.5
    w_up = master_up.astype(jnp.bfloat16)
    w_down = master_down.astype(jnp.bfloat16)
    grad_up, grad_down = mean_grads(inp_rows, out_grad, w_up, w_down)
    true_norm = jnp.sqrt(jnp.sum(grad_up * grad_up) + jnp.sum(grad_down * grad_down))
    clip_frac = jax.random.uniform(keys[4], (), jnp.float32, minval=0.3, maxval=0.7)
    up_size = clip_frac * jnp.sqrt(jnp.mean(grad_up * grad_up, axis=(1, 2), keepdims=True))
    down_size = clip_frac * jnp.sqrt(jnp.mean(grad_down * grad_down, axis=(1, 2), keepdims=True))
    mom_up = (1.0 - BETA1) * up_size * jax.random.normal(keys[5], (2, D, FF), jnp.float32)
    mom_down = (1.0 - BETA1) * down_size * jax.random.normal(keys[6], (2, FF, D), jnp.float32)
    var_up = (1.0 - BETA2) * up_size * up_size * jax.random.uniform(keys[7], (2, D, FF), jnp.float32, minval=0.25, maxval=2.0)
    var_down = (1.0 - BETA2) * down_size * down_size * jax.random.uniform(keys[8], (2, FF, D), jnp.float32, minval=0.25, maxval=2.0)
    return {'inp_rows': inp_rows, 'out_grad': out_grad, 'w_up': w_up, 'w_down': w_down, 'master_up': master_up, 'master_down': master_down, 'mom_up': mom_up, 'mom_down': mom_down, 'var_up': var_up, 'var_down': var_down, 'clip_norm': clip_frac * true_norm}


def reference(inp_rows, out_grad, w_up, w_down, master_up, master_down, mom_up, mom_down, var_up, var_down, clip_norm):
    grad_up, grad_down = mean_grads(inp_rows, out_grad, w_up, w_down)
    grad_norm = jnp.sqrt(jnp.sum(grad_up * grad_up) + jnp.sum(grad_down * grad_down))
    clip_scale = jnp.minimum(1.0, clip_norm / (grad_norm + NORM_EPS))
    master_up_new, mom_up_new, var_up_new = adam_update(grad_up, master_up, mom_up, var_up, clip_scale)
    master_down_new, mom_down_new, var_down_new = adam_update(grad_down, master_down, mom_down, var_down, clip_scale)
    return (master_up_new.astype(jnp.bfloat16), master_down_new.astype(jnp.bfloat16), master_up_new, master_down_new, mom_up_new, mom_down_new, var_up_new, var_down_new, grad_norm)
```

```python
import jax
import jax.numpy as jnp
from jax import lax
from jax.experimental import pallas as pl
from jax.experimental.pallas import tpu as pltpu
from jax.sharding import PartitionSpec as P

BETA1 = 0.9
BETA2 = 0.95
ADAM_EPS = 1e-8
LEARN_RATE = 5e-3
NORM_EPS = 1e-6
STEP = 10
BIAS_ONE = 1.0 - BETA1 ** STEP
BIAS_TWO = 1.0 - BETA2 ** STEP
MESH = pl.DeviceIdType.MESH
F32 = jnp.float32
BF16 = jnp.bfloat16

B, D, FF = 4096, 768, 3072
NB = 6
HB = FF // NB // 2
BF = 2 * HB
R = 1024
NCH = B // R
STEPS = 2 * NB
SLOTS = 3
SQRT_HALF = 0.7071067811865476
PDF_SCALE = 0.3989422804014327


def gelu_value(pre_act):
    return pre_act * (0.5 + 0.5 * lax.erf(pre_act * SQRT_HALF))


def dot(a, b, dims):
    return lax.dot_general(a, b, (dims, ((), ())), preferred_element_type=F32)


class Item:
    def __init__(self, rows, cols, refs, sems):
        self.rows, self.cols = rows, cols
        self.acc, self.r0, self.r1, self.r2, self.hh = refs
        self.send, self.recv, self.loc = sems


def mega_kernel(h_hbm, dy_hbm, x_hbm, z_hbm, wu_hbm, wd_hbm,
                gup, gdn, ssq,
                abuf, bbuf, cbuf, wa, wb, zb, slope,
                acc_d, r0_d, r1_d, r2_d, h_d,
                acc_u, r0_u, r1_u, r2_u, h_u,
                asem, bsem, wsem, zsem,
                send_d, recv_d, loc_d, send_u, recv_u, loc_u):
    r = lax.axis_index('replica')
    d = lax.axis_index('data')
    x = lax.rem(r, 2)
    y = lax.div(r, 2)
    x_off = 1 - 2 * x
    y_off = 2 - 4 * y
    partner = (r, 1 - d)
    n1 = (r + (1 - d) * x_off + d * y_off, d)
    n2 = (r + (1 - d) * y_off + d * x_off, d)
    a = (1 - d) * x + d * y
    b = (1 - d) * y + d * x

    item_d = Item(HB, D, (acc_d, r0_d, r1_d, r2_d, h_d), (send_d, recv_d, loc_d))
    item_u = Item(D // 2, BF, (acc_u, r0_u, r1_u, r2_u, h_u), (send_u, recv_u, loc_u))

    def rows_of(start, size):
        return pl.ds(pl.multiple_of(start, 8), size)

    def row_copy(src, dst, sem, i):
        rows = rows_of(i * R, R)
        return pltpu.make_async_copy(src.at[rows, :], dst.at[rows, :], sem.at[i])

    def w_copies(s):
        slot = lax.rem(s, 2)
        j = lax.rem(s, NB)
        ph = 1 - lax.div(s, NB)
        up, down = [], []
        for p in range(2):
            cols = pl.ds(pl.multiple_of(p * (FF // 2) + j * HB, 128), HB)
            up.append(pltpu.make_async_copy(wu_hbm.at[1, :, cols], wa.at[slot, :, p * HB:(p + 1) * HB], wsem.at[slot, p]))
            down.append(pltpu.make_async_copy(wd_hbm.at[ph, cols, :], wb.at[slot, p * HB:(p + 1) * HB, :], wsem.at[slot, 2 + p]))
        return up, down

    def z_copies(j, i):
        slot = lax.rem(i, 2)
        out = []
        for p in range(2):
            cols = pl.ds(pl.multiple_of(p * (FF // 2) + j * HB, 128), HB)
            out.append(pltpu.make_async_copy(z_hbm.at[rows_of(i * R, R), cols], zb.at[slot, :, p * HB:(p + 1) * HB], zsem.at[slot, p]))
        return out

    def g_rows(it, s, part, size):
        w = 1 - lax.div(s, NB)
        j = lax.rem(s, NB)
        if it is item_d:
            return gdn.at[w, rows_of(j * HB + part, size), :]
        return gup.at[w, j, rows_of(part, size), :]

    def cp(it, stage, s):
        k = lax.rem(s, SLOTS)
        rows = it.rows
        half, quarter = rows // 2, rows // 4
        if stage == 0:
            src, dst, dev = it.acc.at[rows_of((1 - d) * rows, rows), :], it.r0.at[k], partner
        elif stage == 1:
            src, dst, dev = it.r0.at[k, rows_of((1 - a) * half, half), :], it.r1.at[k], n1
        elif stage == 2:
            src, dst, dev = it.r1.at[k, rows_of((1 - b) * quarter, quarter), :], it.r2.at[k], n2
        elif stage == 3:
            q = rows_of(b * quarter, quarter)
            src, dst, dev = it.hh.at[k, q, :], it.hh.at[k, q, :], n2
        else:
            src, dst, dev = it.hh.at[k], g_rows(it, s, a * half, half), n1
        return pltpu.make_async_remote_copy(src_ref=src, dst_ref=dst, send_sem=it.send.at[stage, k],
                                            recv_sem=it.recv.at[stage, k], device_id=dev, device_id_type=MESH)

    def local_out(it, s):
        k = lax.rem(s, SLOTS)
        half = it.rows // 2
        return pltpu.make_async_copy(it.hh.at[k], g_rows(it, s, a * half, half), it.loc.at[k])

    def fold(it, stage, s):
        k = lax.rem(s, SLOTS)
        rows = it.rows
        half, quarter = rows // 2, rows // 4
        if stage == 0:
            return
        cp(it, stage - 1, s).wait()
        if stage == 1:
            it.r0[k] = it.r0[k] + it.acc[rows_of(d * rows, rows), :]
        elif stage == 2:
            it.r1[k] = it.r1[k] + it.r0[k, rows_of(a * half, half), :]
        elif stage == 3:
            g = (it.r2[k] + it.r1[k, rows_of(b * quarter, quarter), :]) * 0.125
            it.hh[k, rows_of(b * quarter, quarter), :] = g
            sq = g * g
            sq = sq.reshape(quarter // 8, 8, it.cols).sum(axis=0)
            tot = sq[:, :128]
            for c in range(1, it.cols // 128):
                tot = tot + sq[:, c * 128:(c + 1) * 128]
            ssq[...] += tot
        elif stage == 5:
            local_out(it, s).wait()

    def post(it, stage, s):
        if stage < 5:
            cp(it, stage, s).start()
        if stage == 4:
            local_out(it, s).start()

    def tick(s, plan):
        late = None
        for it, stage, lag in plan:
            t = s - lag
            ok = jnp.logical_and(t >= 0, t < STEPS)

            @pl.when(ok)
            def _():
                fold(it, stage, t)

            if late is not None:
                pit, pstage, pt, pok = late

                @pl.when(pok)
                def _():
                    post(pit, pstage, pt)
            late = (it, stage, t, ok)
        pit, pstage, pt, pok = late

        @pl.when(pok)
        def _():
            post(pit, pstage, pt)

    ssq[...] = jnp.zeros_like(ssq)
    for i in range(NCH):
        row_copy(h_hbm, abuf, asem, i).start()
        row_copy(dy_hbm, bbuf, bsem, i).start()
        if i == 0:
            up, down = w_copies(0)
            for c in up + down:
                c.start()

    barrier = pltpu.get_barrier_semaphore()
    for dev in (partner, n1, n2):
        pl.semaphore_signal(barrier, inc=1, device_id=dev, device_id_type=MESH)
    pl.semaphore_wait(barrier, 3)

    def zero_c(i, carry):
        cbuf[rows_of(i * 128, 128), :] = jnp.zeros((128, D), F32)
        return carry
    lax.fori_loop(0, B // 128, zero_c, 0)

    def pass_one(s):
        slot = lax.rem(s, 2)
        j = lax.rem(s, NB)
        acc_d[...] = jnp.zeros_like(acc_d)

        def chunk(i, carry):
            rows = rows_of(i * R, R)
            zs = lax.rem(i, 2)

            @pl.when(s == 0)
            def _():
                row_copy(h_hbm, abuf, asem, i).wait()
                row_copy(dy_hbm, bbuf, bsem, i).wait()

            @pl.when(s < NB)
            def _():
                zb[zs] = dot(abuf[rows, :], wa[slot], ((1,), (0,))).astype(BF16)

            @pl.when(s >= NB)
            def _():
                for c in z_copies(j, i):
                    c.wait()

                @pl.when(i + 1 < NCH)
                def _():
                    for c in z_copies(j, i + 1):
                        c.start()

            z = zb[zs].astype(F32)
            cdf = 0.5 + 0.5 * lax.erf(z * SQRT_HALF)
            slope[rows, :] = cdf + z * jnp.exp(-0.5 * z * z) * PDF_SCALE
            u = (z * cdf).astype(BF16)
            acc_d[...] += dot(u, bbuf[rows, :], ((0,), (0,)))
            return carry
        lax.fori_loop(0, NCH, chunk, 0)

    def pass_two(s):
        slot = lax.rem(s, 2)
        acc_u[...] = jnp.zeros_like(acc_u)

        def chunk(i, carry):
            rows = rows_of(i * R, R)

            @pl.when(s == NB)
            def _():
                row_copy(x_hbm, abuf, asem, i).wait()
            e = dot(bbuf[rows, :], wb[slot], ((1,), (1,))).astype(BF16)
            dd = (e.astype(F32) * slope[rows, :]).astype(BF16)
            acc_u[...] += dot(abuf[rows, :], dd, ((0,), (0,)))

            @pl.when(s < NB)
            def _():
                cbuf[rows, :] += dot(dd, wa[slot], ((1,), (1,)))
            return carry
        lax.fori_loop(0, NCH, chunk, 0)

    def step(s, carry):
        @pl.when(s == NB)
        def _():
            for i in range(NCH):
                row_copy(x_hbm, abuf, asem, i).start()

            def conv(i, carry):
                rows = rows_of(i * 128, 128)
                bbuf[rows, :] = cbuf[rows, :].astype(BF16)
                return carry
            lax.fori_loop(0, B // 128, conv, 0)

        @pl.when(s < STEPS)
        def _():
            up, down = w_copies(s)
            for c in down:
                c.wait()

            @pl.when(s < NB)
            def _():
                for c in up:
                    c.wait()

            @pl.when(s >= NB)
            def _():
                for c in z_copies(lax.rem(s, NB), 0):
                    c.start()

            @pl.when(s + 1 < STEPS)
            def _():
                up, down = w_copies(s + 1)
                for c in down:
                    c.start()

                @pl.when(s + 1 < NB)
                def _():
                    for c in up:
                        c.start()
            pass_one(s)

        tick(s, [(item_d, 2, 1), (item_u, 1, 1), (item_u, 3, 2), (item_d, 4, 2), (item_u, 5, 3), (item_d, 0, 0)])

        @pl.when(s < STEPS)
        def _():
            pass_two(s)

        tick(s, [(item_u, 2, 1), (item_d, 1, 0), (item_d, 3, 1), (item_u, 4, 2), (item_d, 5, 2), (item_u, 0, 0)])
        return carry

    lax.fori_loop(0, STEPS + 3, step, 0)


def backward_reduce(h, dy, x, z1, w_up, w_down):
    any_spec = pl.BlockSpec(memory_space=pl.ANY)
    vmem = pltpu.VMEM

    def item(rows, cols, acc):
        return [vmem(acc, F32), vmem((SLOTS, rows, cols), F32), vmem((SLOTS, rows // 2, cols), F32),
                vmem((SLOTS, rows // 4, cols), F32), vmem((SLOTS, rows // 2, cols), F32)]
    dma = pltpu.SemaphoreType.DMA
    return pl.pallas_call(
        mega_kernel,
        out_shape=(jax.ShapeDtypeStruct((2, NB, D // 2, BF), F32),
                   jax.ShapeDtypeStruct((2, FF // 2, D), F32),
                   jax.ShapeDtypeStruct((8, 128), F32)),
        in_specs=[any_spec] * 6,
        out_specs=(any_spec, any_spec, pl.BlockSpec(memory_space=pltpu.VMEM)),
        scratch_shapes=[vmem((B, D), BF16), vmem((B, D), BF16), vmem((B, D), F32),
                        vmem((2, D, BF), BF16), vmem((2, BF, D), BF16), vmem((2, R, BF), BF16), vmem((B, BF), F32)]
        + item(HB, D, (BF, D)) + item(D // 2, BF, (D, BF))
        + [dma((NCH,)), dma((NCH,)), dma((2, 4)), dma((2, 2))]
        + [dma((5, SLOTS)), dma((5, SLOTS)), dma((SLOTS,))] * 2,
        compiler_params=pltpu.CompilerParams(collective_id=0, has_side_effects=True, vmem_limit_bytes=67043328),
        name='backward_reduce',
    )(h, dy, x, z1, w_up, w_down)


def adam_body(scale_ref, g_ref, master_ref, mom_ref, var_ref, new_master_ref, new_mom_ref, new_var_ref, w_ref):
    s = scale_ref[0]
    g = g_ref[...].reshape(master_ref.shape)
    mom = BETA1 * mom_ref[...] + (1.0 - BETA1) * s * g
    var = BETA2 * var_ref[...] + (1.0 - BETA2) * (s * s) * (g * g)
    master = master_ref[...] - LEARN_RATE * (mom / BIAS_ONE) / (jnp.sqrt(var / BIAS_TWO) + ADAM_EPS)
    new_mom_ref[...] = mom
    new_var_ref[...] = var
    new_master_ref[...] = master
    w_ref[...] = master.astype(BF16)


def adam(scale, g, master, mom, var, up):
    if up:
        block = (1, D // 2, HB)
        spec = pl.BlockSpec(block, lambda w, j, p: (w, 0, p * NB + j))
        g_spec = pl.BlockSpec((1, 1, D // 2, HB), lambda w, j, p: (w, j, 0, p))
        grid = (2, NB, 2)
    else:
        block = (1, 256, D)
        spec = pl.BlockSpec(block, lambda w, j: (w, j, 0))
        g_spec = spec
        grid = (2, FF // 2 // 256)
    f32 = jax.ShapeDtypeStruct(master.shape, F32)
    return pl.pallas_call(
        adam_body,
        grid=grid,
        out_shape=(f32, f32, f32, jax.ShapeDtypeStruct(master.shape, BF16)),
        in_specs=[pl.BlockSpec(memory_space=pltpu.SMEM), g_spec, spec, spec, spec],
        out_specs=(spec, spec, spec, spec),
        compiler_params=pltpu.CompilerParams(vmem_limit_bytes=48 * 1024 * 1024),
        name='adam_up' if up else 'adam_down',
    )(scale, g, master, mom, var)


def solution(mesh):
    batch_spec = P(('replica', 'data'), None)
    whole_spec = P()
    shard_spec = P(None, 'data', None)

    def device_step(inp_rows, out_grad, w_up, w_down, master_up, master_down, mom_up, mom_down, var_up, var_down, clip_norm):
        pre_one = jnp.dot(inp_rows, w_up[0], preferred_element_type=F32).astype(BF16)
        act_one = gelu_value(pre_one.astype(F32)).astype(BF16)
        mid_rows = jnp.dot(act_one, w_down[0], preferred_element_type=F32).astype(BF16)
        g_up, g_down, squares = backward_reduce(mid_rows, out_grad, inp_rows, pre_one, w_up, w_down)
        grad_norm = jnp.sqrt(lax.psum(jnp.sum(squares), ('replica', 'data')))
        clip_scale = jnp.minimum(1.0, clip_norm / (grad_norm + NORM_EPS))
        scale = clip_scale.reshape(1)
        master_up_new, mom_up_new, var_up_new, w_up_half = adam(scale, g_up, master_up, mom_up, var_up, True)
        master_down_new, mom_down_new, var_down_new, w_down_half = adam(scale, g_down, master_down, mom_down, var_down, False)
        w_up_new = lax.all_gather(w_up_half, 'data', axis=1, tiled=True)
        w_down_new = lax.all_gather(w_down_half, 'data', axis=1, tiled=True)
        return (w_up_new, w_down_new, master_up_new, master_down_new, mom_up_new, mom_down_new, var_up_new, var_down_new, grad_norm)

    return jax.shard_map(device_step, mesh=mesh, in_specs=(batch_spec, batch_spec, whole_spec, whole_spec, shard_spec, shard_spec, shard_spec, shard_spec, shard_spec, shard_spec, whole_spec), out_specs=(whole_spec, whole_spec, shard_spec, shard_spec, shard_spec, shard_spec, shard_spec, shard_spec, whole_spec), check_vma=False)
```

```python
import jax
import jax.numpy as jnp
from jax import lax
from jax.experimental import pallas as pl
from jax.experimental.pallas import tpu as pltpu
from jax.sharding import PartitionSpec as P


BETA1 = 0.9
BETA2 = 0.95
ADAM_EPS = 1e-8
LEARN_RATE = 5e-3
NORM_EPS = 1e-6
STEP = 10
BIAS_ONE = 1.0 - BETA1 ** STEP
BIAS_TWO = 1.0 - BETA2 ** STEP
MESH = pl.DeviceIdType.MESH
F32 = jnp.float32
BF16 = jnp.bfloat16

B, D, FF = 4096, 768, 3072
NB = 6
HB = FF // NB // 2
BF = 2 * HB
R = 1024
NCH = B // R
STEPS = 2 * NB
SLOTS = 3
TAIL = 2
FULL = STEPS - TAIL
SQRT_HALF = 0.7071067811865476
PDF_SCALE = 0.3989422804014327


def gelu_value(pre_act):
    return pre_act * (0.5 + 0.5 * lax.erf(pre_act * SQRT_HALF))


def dot(a, b, dims):
    return lax.dot_general(a, b, (dims, ((), ())), preferred_element_type=F32)


class Item:
    def __init__(self, rows, cols, refs, sems):
        self.rows, self.cols = rows, cols
        self.acc, self.r0, self.r1, self.r2, self.hh = refs
        self.send, self.recv, self.loc = sems


def mega_kernel(clip_ref, h_hbm, dy_hbm, x_hbm, z_hbm, wu_hbm, wd_hbm,
                gup, gdn, gtail, stats,
                abuf, bbuf, cbuf, wa, wb, zb, slope,
                acc_d, r0_d, r1_d, r2_d, h_d,
                acc_u, r0_u, r1_u, r2_u, h_u,
                ssq, sq_in, asem, bsem, wsem, zsem, tsem, nsend, nrecv,
                send_d, recv_d, loc_d, send_u, recv_u, loc_u):
    r = lax.axis_index('replica')
    d = lax.axis_index('data')
    x = lax.rem(r, 2)
    y = lax.div(r, 2)
    x_off = 1 - 2 * x
    y_off = 2 - 4 * y
    partner = (r, 1 - d)
    n1 = (r + (1 - d) * x_off + d * y_off, d)
    n2 = (r + (1 - d) * y_off + d * x_off, d)
    a = (1 - d) * x + d * y
    b = (1 - d) * y + d * x

    item_d = Item(HB, D, (acc_d, r0_d, r1_d, r2_d, h_d), (send_d, recv_d, loc_d))
    item_u = Item(D // 2, BF, (acc_u, r0_u, r1_u, r2_u, h_u), (send_u, recv_u, loc_u))

    def rows_of(start, size):
        return pl.ds(pl.multiple_of(start, 8), size)

    def row_copy(src, dst, sem, i):
        rows = rows_of(i * R, R)
        return pltpu.make_async_copy(src.at[rows, :], dst.at[rows, :], sem.at[i])

    def w_copies(s):
        slot = lax.rem(s, 2)
        j = lax.rem(s, NB)
        ph = 1 - lax.div(s, NB)
        up, down = [], []
        for p in range(2):
            cols = pl.ds(pl.multiple_of(p * (FF // 2) + j * HB, 128), HB)
            up.append(pltpu.make_async_copy(wu_hbm.at[1, :, cols], wa.at[slot, :, p * HB:(p + 1) * HB], wsem.at[slot, p]))
            down.append(pltpu.make_async_copy(wd_hbm.at[ph, cols, :], wb.at[slot, p * HB:(p + 1) * HB, :], wsem.at[slot, 2 + p]))
        return up, down

    def z_copies(j, i):
        slot = lax.rem(i, 2)
        out = []
        for p in range(2):
            cols = pl.ds(pl.multiple_of(p * (FF // 2) + j * HB, 128), HB)
            out.append(pltpu.make_async_copy(z_hbm.at[rows_of(i * R, R), cols], zb.at[slot, :, p * HB:(p + 1) * HB], zsem.at[slot, p]))
        return out

    def g_rows(it, s, part, size):
        w = 1 - lax.div(s, NB)
        j = lax.rem(s, NB)
        if it is item_d:
            return gdn.at[w, rows_of(j * HB + part, size), :]
        return gup.at[w, j, rows_of(part, size), :]

    def cp(it, stage, s):
        k = lax.rem(s, SLOTS)
        rows = it.rows
        half, quarter = rows // 2, rows // 4
        if stage == 0:
            src, dst, dev = it.acc.at[rows_of((1 - d) * rows, rows), :], it.r0.at[k], partner
        elif stage == 1:
            src, dst, dev = it.r0.at[k, rows_of((1 - a) * half, half), :], it.r1.at[k], n1
        elif stage == 2:
            src, dst, dev = it.r1.at[k, rows_of((1 - b) * quarter, quarter), :], it.r2.at[k], n2
        elif stage == 3:
            q = rows_of(b * quarter, quarter)
            src, dst, dev = it.hh.at[k, q, :], it.hh.at[k, q, :], n2
        else:
            src, dst, dev = it.hh.at[k], g_rows(it, s, a * half, half), n1
        return pltpu.make_async_remote_copy(src_ref=src, dst_ref=dst, send_sem=it.send.at[stage, k],
                                            recv_sem=it.recv.at[stage, k], device_id=dev, device_id_type=MESH)

    def local_out(it, s):
        k = lax.rem(s, SLOTS)
        half = it.rows // 2
        return pltpu.make_async_copy(it.hh.at[k], g_rows(it, s, a * half, half), it.loc.at[k])

    def fold(it, stage, s):
        k = lax.rem(s, SLOTS)
        rows = it.rows
        half, quarter = rows // 2, rows // 4
        if stage == 0:
            return
        cp(it, stage - 1, s).wait()
        if stage == 1:
            it.r0[k] = it.r0[k] + it.acc[rows_of(d * rows, rows), :]
        elif stage == 2:
            it.r1[k] = it.r1[k] + it.r0[k, rows_of(a * half, half), :]
        elif stage == 3:
            g = (it.r2[k] + it.r1[k, rows_of(b * quarter, quarter), :]) * 0.125
            it.hh[k, rows_of(b * quarter, quarter), :] = g
            sq = g * g
            sq = sq.reshape(quarter // 8, 8, it.cols).sum(axis=0)
            tot = sq[:, :128]
            for c in range(1, it.cols // 128):
                tot = tot + sq[:, c * 128:(c + 1) * 128]
            ssq[0] += tot
        elif stage == 5:
            local_out(it, s).wait()

    def tail_out(it, s):
        k = lax.rem(s, SLOTS)
        quarter = it.rows // 4
        ty = 0 if it is item_d else 1
        return [pltpu.make_async_copy(it.hh.at[k, rows_of(b * quarter, quarter), p * 256:(p + 1) * 256],
                                      gtail.at[s - FULL, ty, p * quarter:(p + 1) * quarter, :],
                                      tsem.at[s - FULL, ty, p]) for p in range(it.cols // 256)]

    def post(it, stage, s):
        if stage == 3:
            @pl.when(s < FULL)
            def _():
                cp(it, 3, s).start()

            @pl.when(s >= FULL)
            def _():
                for c in tail_out(it, s):
                    c.start()
        elif stage < 5:
            cp(it, stage, s).start()
        if stage == 4:
            local_out(it, s).start()

    def tick(s, plan):
        late = None
        for it, stage, lag in plan:
            t = s - lag
            ok = jnp.logical_and(t >= 0, t < (FULL if stage >= 4 else STEPS))

            @pl.when(ok)
            def _():
                fold(it, stage, t)

            if late is not None:
                pit, pstage, pt, pok = late

                @pl.when(pok)
                def _():
                    post(pit, pstage, pt)
            late = (it, stage, t, ok)
        pit, pstage, pt, pok = late

        @pl.when(pok)
        def _():
            post(pit, pstage, pt)

    ssq[0] = jnp.zeros((8, 128), F32)
    for i in range(NCH):
        row_copy(h_hbm, abuf, asem, i).start()
        row_copy(dy_hbm, bbuf, bsem, i).start()
        if i == 0:
            up, down = w_copies(0)
            for c in up + down:
                c.start()

    barrier = pltpu.get_barrier_semaphore()
    for dev in (partner, n1, n2):
        pl.semaphore_signal(barrier, inc=1, device_id=dev, device_id_type=MESH)
    pl.semaphore_wait(barrier, 3)

    def zero_c(i, carry):
        cbuf[rows_of(i * 128, 128), :] = jnp.zeros((128, D), F32)
        return carry

    lax.fori_loop(0, B // 128, zero_c, 0)

    def pass_one(s):
        slot = lax.rem(s, 2)
        j = lax.rem(s, NB)
        acc_d[...] = jnp.zeros_like(acc_d)

        def chunk(i, carry):
            rows = rows_of(i * R, R)
            zs = lax.rem(i, 2)

            @pl.when(s == 0)
            def _():
                row_copy(h_hbm, abuf, asem, i).wait()
                row_copy(dy_hbm, bbuf, bsem, i).wait()

            @pl.when(s < NB)
            def _():
                zb[zs] = dot(abuf[rows, :], wa[slot], ((1,), (0,))).astype(BF16)

            @pl.when(s >= NB)
            def _():
                for c in z_copies(j, i):
                    c.wait()

                @pl.when(i + 1 < NCH)
                def _():
                    for c in z_copies(j, i + 1):
                        c.start()

            z = zb[zs].astype(F32)
            cdf = 0.5 + 0.5 * lax.erf(z * SQRT_HALF)
            slope[rows, :] = cdf + z * jnp.exp(-0.5 * z * z) * PDF_SCALE
            u = (z * cdf).astype(BF16)
            acc_d[...] += dot(u, bbuf[rows, :], ((0,), (0,)))
            return carry

        lax.fori_loop(0, NCH, chunk, 0)

    def pass_two(s):
        slot = lax.rem(s, 2)
        acc_u[...] = jnp.zeros_like(acc_u)

        def chunk(i, carry):
            rows = rows_of(i * R, R)

            @pl.when(s == NB)
            def _():
                row_copy(x_hbm, abuf, asem, i).wait()

            e = dot(bbuf[rows, :], wb[slot], ((1,), (1,))).astype(BF16)
            dd = (e.astype(F32) * slope[rows, :]).astype(BF16)
            acc_u[...] += dot(abuf[rows, :], dd, ((0,), (0,)))

            @pl.when(s < NB)
            def _():
                cbuf[rows, :] += dot(dd, wa[slot], ((1,), (1,)))

            return carry

        lax.fori_loop(0, NCH, chunk, 0)

    def step(s, carry):
        @pl.when(s == NB)
        def _():
            for i in range(NCH):
                row_copy(x_hbm, abuf, asem, i).start()

            def conv(i, carry):
                rows = rows_of(i * 128, 128)
                bbuf[rows, :] = cbuf[rows, :].astype(BF16)
                return carry

            lax.fori_loop(0, B // 128, conv, 0)

        @pl.when(s < STEPS)
        def _():
            up, down = w_copies(s)
            for c in down:
                c.wait()

            @pl.when(s < NB)
            def _():
                for c in up:
                    c.wait()

            @pl.when(s >= NB)
            def _():
                for c in z_copies(lax.rem(s, NB), 0):
                    c.start()

            @pl.when(s + 1 < STEPS)
            def _():
                up, down = w_copies(s + 1)
                for c in down:
                    c.start()

                @pl.when(s + 1 < NB)
                def _():
                    for c in up:
                        c.start()

            pass_one(s)

        tick(s, [(item_d, 2, 1), (item_u, 1, 1), (item_u, 3, 2), (item_d, 4, 2), (item_u, 5, 3), (item_d, 0, 0)])

        @pl.when(s < STEPS)
        def _():
            pass_two(s)

        tick(s, [(item_u, 2, 1), (item_d, 1, 0), (item_d, 3, 1), (item_u, 4, 2), (item_d, 5, 2), (item_u, 0, 0)])
        return carry

    lax.fori_loop(0, STEPS + 2, step, 0)

    for i, dev in enumerate((partner, (r + x_off, d), (r + y_off, d))):
        c = pltpu.make_async_remote_copy(src_ref=ssq.at[i], dst_ref=sq_in.at[i], send_sem=nsend.at[i],
                                         recv_sem=nrecv.at[i], device_id=dev, device_id_type=MESH)
        c.start()
        if i == 0:
            for t in range(FULL, STEPS):
                for it in (item_d, item_u):
                    for tc in tail_out(it, t):
                        tc.wait()
        c.wait()
        ssq[i + 1] = ssq[i] + sq_in[i]
    total = jnp.sum(ssq[3], axis=0, keepdims=True)
    total = jnp.sum(total, axis=1, keepdims=True)
    norm = jnp.sqrt(total)
    scale = jnp.minimum(1.0, clip_ref[0] / (norm + NORM_EPS))
    stats[0] = jnp.broadcast_to(norm, (8, 128))
    stats[1] = jnp.broadcast_to(scale, (8, 128))


def backward_reduce(clip, h, dy, x, z1, w_up, w_down):
    any_spec = pl.BlockSpec(memory_space=pl.ANY)
    vmem = pltpu.VMEM

    def item(rows, cols, acc):
        return [vmem(acc, F32), vmem((SLOTS, rows, cols), F32), vmem((SLOTS, rows // 2, cols), F32),
                vmem((SLOTS, rows // 4, cols), F32), vmem((SLOTS, rows // 2, cols), F32)]

    dma = pltpu.SemaphoreType.DMA
    return pl.pallas_call(
        mega_kernel,
        out_shape=(jax.ShapeDtypeStruct((2, NB, D // 2, BF), F32),
                   jax.ShapeDtypeStruct((2, FF // 2, D), F32),
                   jax.ShapeDtypeStruct((TAIL, 2, 192, 256), F32),
                   jax.ShapeDtypeStruct((2, 8, 128), F32)),
        in_specs=[pl.BlockSpec(memory_space=pltpu.SMEM)] + [any_spec] * 6,
        out_specs=(any_spec, any_spec, any_spec, pl.BlockSpec(memory_space=pltpu.VMEM)),
        scratch_shapes=[vmem((B, D), BF16), vmem((B, D), BF16), vmem((B, D), F32),
                        vmem((2, D, BF), BF16), vmem((2, BF, D), BF16), vmem((2, R, BF), BF16), vmem((B, BF), F32)]
        + item(HB, D, (BF, D)) + item(D // 2, BF, (D, BF))
        + [vmem((4, 8, 128), F32), vmem((3, 8, 128), F32)]
        + [dma((NCH,)), dma((NCH,)), dma((2, 4)), dma((2, 2)), dma((TAIL, 2, 3)), dma((3,)), dma((3,))]
        + [dma((5, SLOTS)), dma((5, SLOTS)), dma((SLOTS,))] * 2,
        compiler_params=pltpu.CompilerParams(collective_id=0, has_side_effects=True, vmem_limit_bytes=67043328),
        name='backward_reduce',
    )(clip, h, dy, x, z1, w_up, w_down)


def adam_rule(s, g, master_ref, mom_ref, var_ref, new_master_ref, new_mom_ref, new_var_ref, w_ref):
    mom = BETA1 * mom_ref[0] + (1.0 - BETA1) * s * g
    var = BETA2 * var_ref[0] + (1.0 - BETA2) * (s * s) * (g * g)
    master = master_ref[0] - LEARN_RATE * (mom / BIAS_ONE) / (jnp.sqrt(var / BIAS_TWO) + ADAM_EPS)
    new_mom_ref[0] = mom
    new_var_ref[0] = var
    new_master_ref[0] = master
    w_ref[0] = master.astype(BF16)


def adam_body(tail, n_alias, stats, *refs):
    s = stats[1, 0:1, 0:1]
    if tail:
        own, from_n2, from_n1, from_diag = refs[:4]
        refs = refs[4:]
        r = lax.axis_index('replica')
        d = lax.axis_index('data')
        x, y = lax.rem(r, 2), lax.div(r, 2)
        a = (1 - d) * x + d * y
        b = (1 - d) * y + d * x
        i = pl.program_id(0)
        half = lax.rem(i, 2)

        def pick(qa, qb, ty, rows):
            da = lax.rem(qa + a, 2)
            db = lax.rem(qb + b, 2)
            near = jnp.where(db == 0, own[0, ty, rows, :], from_n2[0, ty, rows, :])
            far = jnp.where(db == 0, from_n1[0, ty, rows, :], from_diag[0, ty, rows, :])
            return jnp.where(da == 0, near, far)

        up_rows = pl.ds(pl.multiple_of(half * 96, 8), 96)
        g_up = jnp.concatenate([pick(q // 2, q % 2, 1, up_rows) for q in range(4)], axis=0)
        g_down = jnp.concatenate([jnp.concatenate([pick(half, qb, 0, pl.ds(p * 64, 64)) for p in range(3)], axis=1)
                                  for qb in range(2)], axis=0)
    else:
        g_up = refs[0][0, 0]
        g_down = refs[1][0]
        refs = refs[2:]
    states, outs = refs[:6], refs[6 + n_alias:]
    adam_rule(s, g_up, *states[:3], *outs[:3], outs[6])
    adam_rule(s, g_down, *states[3:], *outs[3:6], outs[7])


def adam(stats, grads, states, prev, w, lo, hi, tail=False):
    any_spec = pl.BlockSpec(memory_space=pl.ANY)
    up = pl.BlockSpec((1, D // 2, HB), lambda i: (w, 0, lax.rem(i + lo, 2) * NB + lax.div(i + lo, 2)))
    down = pl.BlockSpec((1, 128, D), lambda i: (w, i + lo, 0))
    if tail:
        g_specs = [pl.BlockSpec((1, 2, 192, 256), lambda i: (lax.div(i, 2), 0, 0, 0))] * 4
    else:
        g_specs = [pl.BlockSpec((1, 1, D // 2, HB), lambda i: (w, lax.div(i + lo, 2), 0, lax.rem(i + lo, 2))), down]
    n = hi - lo
    full = [jax.ShapeDtypeStruct(v.shape, F32) for v in states]
    halves = [jax.ShapeDtypeStruct((n, D // 2, HB), BF16), jax.ShapeDtypeStruct((n, 128, D), BF16)]
    first = 1 + len(grads) + 6
    cells = n * (D // 2 * HB + 128 * D)
    return pl.pallas_call(
        lambda *refs: adam_body(tail, len(prev), *refs),
        grid=(n,),
        out_shape=full + halves,
        in_specs=[pl.BlockSpec((2, 8, 128), lambda i: (0, 0, 0))] + g_specs + [up] * 3 + [down] * 3 + [any_spec] * len(prev),
        out_specs=[up] * 3 + [down] * 3 + [pl.BlockSpec((1, D // 2, HB), lambda i: (i, 0, 0)), pl.BlockSpec((1, 128, D), lambda i: (i, 0, 0))],
        input_output_aliases={first + k: k for k in range(len(prev))},
        compiler_params=pltpu.CompilerParams(vmem_limit_bytes=67043328),
        cost_estimate=pl.CostEstimate(flops=cells * 400, bytes_accessed=cells * 30, transcendentals=0),
    )(stats, *grads, *states, *prev)


def place_kernel(w, lo, n, n_extra, own_u, own_d, got_u, got_d, *rest):
    out_u, out_d, buf_u, buf_d, sem_in, sem_out = rest[n_extra:]
    d = lax.axis_index('data')
    loads, stores = [], []
    for k, (src_u, src_d) in enumerate(((own_u, own_d), (got_u, got_d))):
        q = d if k == 0 else 1 - d
        loads.append(pltpu.make_async_copy(src_u, buf_u.at[k], sem_in.at[k, 0]))
        loads.append(pltpu.make_async_copy(src_d, buf_d.at[k], sem_in.at[k, 1]))
        for i in range(n):
            t = i + lo
            cols = pl.ds(((t % 2) * NB + t // 2) * HB, HB)
            stores.append((2 * k, pltpu.make_async_copy(
                buf_u.at[k, i], out_u.at[w, pl.ds(pl.multiple_of(q * (D // 2), 8), D // 2), cols], sem_out.at[k, i])))
            rows = pl.ds(pl.multiple_of(q * (FF // 2) + t * 128, 8), 128)
            stores.append((2 * k + 1, pltpu.make_async_copy(buf_d.at[k, i], out_d.at[w, rows, :], sem_out.at[k, n + i])))
    for c in loads:
        c.start()
    for k, c in enumerate(loads):
        c.wait()
        for kk, st in stores:
            if kk == k:
                st.start()
    for kk, st in stores:
        st.wait()


def place(w, lo, own, got, prev, after):
    n = own[0].shape[0]
    any_spec = pl.BlockSpec(memory_space=pl.ANY)
    extra = list(prev) + list(after)
    cells = 2 * n * (D // 2 * HB + 128 * D)
    return pl.pallas_call(
        lambda *refs: place_kernel(w, lo, n, len(extra), *refs),
        out_shape=(jax.ShapeDtypeStruct((2, D, FF), BF16), jax.ShapeDtypeStruct((2, FF, D), BF16)),
        in_specs=[any_spec] * (4 + len(extra)),
        out_specs=(any_spec, any_spec),
        scratch_shapes=[pltpu.VMEM((2, n, D // 2, HB), BF16), pltpu.VMEM((2, n, 128, D), BF16),
                        pltpu.SemaphoreType.DMA((2, 2)), pltpu.SemaphoreType.DMA((2, 2 * n))],
        input_output_aliases={4 + k: k for k in range(len(prev))},
        compiler_params=pltpu.CompilerParams(vmem_limit_bytes=67043328),
        cost_estimate=pl.CostEstimate(flops=cells * 100, bytes_accessed=cells * 4, transcendentals=0),
    )(*own, *got, *extra)


def swap(halves):
    return [lax.ppermute(v, 'data', [(0, 1), (1, 0)]) for v in halves]


def solution(mesh):
    batch_spec = P(('replica', 'data'), None)
    whole_spec = P()
    shard_spec = P(None, 'data', None)
    first_axis = [(r * 2 + d, (r ^ (1 if d == 0 else 2)) * 2 + d) for r in range(4) for d in range(2)]
    second_axis = [(r * 2 + d, (r ^ (2 if d == 0 else 1)) * 2 + d) for r in range(4) for d in range(2)]
    both_axes = [(r * 2 + d, (r ^ 3) * 2 + d) for r in range(4) for d in range(2)]

    def device_step(inp_rows, out_grad, w_up, w_down, master_up, master_down, mom_up, mom_down, var_up, var_down, clip_norm):
        pre_one = jnp.dot(inp_rows, w_up[0], preferred_element_type=F32).astype(BF16)
        act_one = gelu_value(pre_one.astype(F32)).astype(BF16)
        mid_rows = jnp.dot(act_one, w_down[0], preferred_element_type=F32).astype(BF16)
        g_up, g_down, g_tail, stats = backward_reduce(clip_norm.reshape(1), mid_rows, out_grad, inp_rows, pre_one, w_up, w_down)
        axes = ('replica', 'data')
        tails = [g_tail]
        for perm in (second_axis, first_axis, both_axes):
            tails.append(lax.ppermute(g_tail, axes, perm))
        states = [master_up, mom_up, var_up, master_down, mom_down, var_down]
        cut = 2 * (NB - TAIL)
        *new, wu, wd = adam(stats, [g_up, g_down], states, [], 1, 0, 2 * NB)
        own_a = [wu, wd]
        got_a = swap(own_a)
        *new, wu, wd = adam(stats, [g_up, g_down], states, new, 0, 0, cut)
        own_b = [wu, wd]
        got_b = swap(own_b)
        weights = place(1, 0, own_a, got_a, [], [wu])
        *new, wu, wd = adam(stats, tails, states, new, 0, cut, 2 * NB, tail=True)
        own_c = [wu, wd]
        got_c = swap(own_c)
        weights = place(0, 0, own_b, got_b, weights, [wu])
        weights = place(0, cut, own_c, got_c, weights, [])
        m_up, o_up, v_up, m_down, o_down, v_down = new
        return (weights[0], weights[1], m_up, m_down, o_up, o_down, v_up, v_down, stats[0, 0, 0])

    return jax.shard_map(device_step, mesh=mesh, in_specs=(batch_spec, batch_spec, whole_spec, whole_spec, shard_spec, shard_spec, shard_spec, shard_spec, shard_spec, shard_spec, whole_spec), out_specs=(whole_spec, whole_spec, shard_spec, shard_spec, shard_spec, shard_spec, shard_spec, shard_spec, whole_spec), check_vma=False)
```

```python
import jax
import jax.numpy as jnp
from jax import lax
from jax.experimental import pallas as pl
from jax.experimental.pallas import tpu as pltpu
from jax.sharding import PartitionSpec as P


BETA1 = 0.9
BETA2 = 0.95
ADAM_EPS = 1e-8
LEARN_RATE = 5e-3
NORM_EPS = 1e-6
STEP = 10
BIAS_ONE = 1.0 - BETA1 ** STEP
BIAS_TWO = 1.0 - BETA2 ** STEP
MESH = pl.DeviceIdType.MESH
F32 = jnp.float32
BF16 = jnp.bfloat16

B, D, FF = 4096, 768, 3072
NB = 6
HB = FF // NB // 2
BF = 2 * HB
R = B // 2
NCH = B // R
STEPS = 2 * NB
SLOTS = 3
TAIL = 3
FULL = STEPS - TAIL
SQRT_HALF = 0.7071067811865476
PDF_SCALE = 0.3989422804014327
EXP_SCALE = -0.5 * 1.4426950408889634


def gelu_value(pre_act):
    return pre_act * (0.5 + 0.5 * lax.erf(pre_act * SQRT_HALF))


def dot(a, b, dims):
    return lax.dot_general(a, b, (dims, ((), ())), preferred_element_type=F32)


class Item:
    def __init__(self, rows, cols, refs, sems):
        self.rows, self.cols = rows, cols
        self.acc, self.r0, self.r1, self.r2, self.hh = refs
        self.send, self.recv, self.loc = sems


def mega_kernel(clip_ref, h_hbm, dy_hbm, x_hbm, z_hbm, wu_hbm, wd_hbm,
                gup, gdn, gtail, stats,
                abuf, bbuf, cbuf, wa, wb, zb,
                acc_d, r0_d, r1_d, r2_d, h_d,
                acc_u, r0_u, r1_u, r2_u, h_u,
                ssq, sq_in, asem, bsem, wsem, zsem, tsem, nsend, nrecv,
                send_d, recv_d, loc_d, send_u, recv_u, loc_u):
    r = lax.axis_index('replica')
    d = lax.axis_index('data')
    x = lax.rem(r, 2)
    y = lax.div(r, 2)
    x_off = 1 - 2 * x
    y_off = 2 - 4 * y
    partner = (r, 1 - d)
    n1 = (r + (1 - d) * x_off + d * y_off, d)
    n2 = (r + (1 - d) * y_off + d * x_off, d)
    a = (1 - d) * x + d * y
    b = (1 - d) * y + d * x

    item_d = Item(HB, D, (acc_d, r0_d, r1_d, r2_d, h_d), (send_d, recv_d, loc_d))
    item_u = Item(D // 2, BF, (acc_u, r0_u, r1_u, r2_u, h_u), (send_u, recv_u, loc_u))

    def rows_of(start, size):
        return pl.ds(pl.multiple_of(start, 8), size)

    def row_copy(src, dst, sem, i):
        rows = rows_of(i * R, R)
        return pltpu.make_async_copy(src.at[rows, :], dst.at[rows, :], sem.at[i])

    def w_copies(s):
        slot = lax.rem(s, 2)
        j = lax.rem(s, NB)
        ph = 1 - lax.div(s, NB)
        up, down = [], []
        for p in range(2):
            cols = pl.ds(pl.multiple_of(p * (FF // 2) + j * HB, 128), HB)
            up.append(pltpu.make_async_copy(wu_hbm.at[1, :, cols], wa.at[slot, :, p * HB:(p + 1) * HB], wsem.at[slot, p]))
            down.append(pltpu.make_async_copy(wd_hbm.at[ph, cols, :], wb.at[slot, p * HB:(p + 1) * HB, :], wsem.at[slot, 2 + p]))
        return up, down

    def z_copies(s, i):
        j = lax.rem(s, NB)
        out = []
        for p in range(2):
            cols = pl.ds(pl.multiple_of(p * (FF // 2) + j * HB, 128), HB)
            rows = rows_of(i * R, R)
            out.append(pltpu.make_async_copy(z_hbm.at[rows, cols], zb.at[rows, p * HB:(p + 1) * HB], zsem.at[i, p]))
        return out

    def g_rows(it, s, part, size):
        w = 1 - lax.div(s, NB)
        j = lax.rem(s, NB)
        if it is item_d:
            return gdn.at[w, rows_of(j * HB + part, size), :]
        return gup.at[w, j, rows_of(part, size), :]

    def cp(it, stage, s):
        k = lax.rem(s, SLOTS)
        rows = it.rows
        half, quarter = rows // 2, rows // 4
        if stage == 0:
            src, dst, dev = it.acc.at[rows_of((1 - d) * rows, rows), :], it.r0.at[k], partner
        elif stage == 1:
            src, dst, dev = it.r0.at[k, rows_of((1 - a) * half, half), :], it.r1.at[k], n1
        elif stage == 2:
            src, dst, dev = it.r1.at[k, rows_of((1 - b) * quarter, quarter), :], it.r2.at[k], n2
        elif stage == 3:
            q = rows_of(b * quarter, quarter)
            src, dst, dev = it.hh.at[k, q, :], it.hh.at[k, q, :], n2
        else:
            src, dst, dev = it.hh.at[k], g_rows(it, s, a * half, half), n1
        return pltpu.make_async_remote_copy(src_ref=src, dst_ref=dst, send_sem=it.send.at[stage, k],
                                            recv_sem=it.recv.at[stage, k], device_id=dev, device_id_type=MESH)

    def local_out(it, s):
        k = lax.rem(s, SLOTS)
        half = it.rows // 2
        return pltpu.make_async_copy(it.hh.at[k], g_rows(it, s, a * half, half), it.loc.at[k])

    def fold(it, stage, s):
        k = lax.rem(s, SLOTS)
        rows = it.rows
        half, quarter = rows // 2, rows // 4
        if stage == 0:
            return
        cp(it, stage - 1, s).wait()
        if stage == 1:
            it.r0[k] = it.r0[k] + it.acc[rows_of(d * rows, rows), :]
        elif stage == 2:
            it.r1[k] = it.r1[k] + it.r0[k, rows_of(a * half, half), :]
        elif stage == 3:
            g = (it.r2[k] + it.r1[k, rows_of(b * quarter, quarter), :]) * 0.125
            it.hh[k, rows_of(b * quarter, quarter), :] = g
            sq = g * g
            sq = sq.reshape(quarter // 8, 8, it.cols).sum(axis=0)
            tot = sq[:, :128]
            for c in range(1, it.cols // 128):
                tot = tot + sq[:, c * 128:(c + 1) * 128]
            ssq[0] += tot
        elif stage == 5:
            local_out(it, s).wait()

    def tail_out(it, s):
        k = lax.rem(s, SLOTS)
        quarter = it.rows // 4
        ty = 0 if it is item_d else 1
        return [pltpu.make_async_copy(it.hh.at[k, rows_of(b * quarter, quarter), p * 256:(p + 1) * 256],
                                      gtail.at[s - FULL, ty, p * quarter:(p + 1) * quarter, :],
                                      tsem.at[s - FULL, ty, p]) for p in range(it.cols // 256)]

    def post(it, stage, s):
        if stage == 3:
            @pl.when(s < FULL)
            def _():
                cp(it, 3, s).start()

            @pl.when(s >= FULL)
            def _():
                for c in tail_out(it, s):
                    c.start()
        elif stage < 5:
            cp(it, stage, s).start()
        if stage == 4:
            local_out(it, s).start()

    def tick(s, plan):
        late = None
        for it, stage, lag in plan:
            t = s - lag
            ok = jnp.logical_and(t >= 0, t < (FULL if stage >= 4 else STEPS))

            @pl.when(ok)
            def _():
                fold(it, stage, t)

            if late is not None:
                pit, pstage, pt, pok = late

                @pl.when(pok)
                def _():
                    post(pit, pstage, pt)
            late = (it, stage, t, ok)
        pit, pstage, pt, pok = late

        @pl.when(pok)
        def _():
            post(pit, pstage, pt)

    ssq[0] = jnp.zeros((8, 128), F32)
    for i in range(NCH):
        row_copy(h_hbm, abuf, asem, i).start()
        row_copy(dy_hbm, bbuf, bsem, i).start()
        if i == 0:
            up, down = w_copies(0)
            for c in up + down:
                c.start()

    barrier = pltpu.get_barrier_semaphore()
    for dev in (partner, n1, n2):
        pl.semaphore_signal(barrier, inc=1, device_id=dev, device_id_type=MESH)
    pl.semaphore_wait(barrier, 3)

    def zero_c(i, carry):
        cbuf[rows_of(i * 128, 128), :] = jnp.zeros((128, D), F32)
        return carry

    lax.fori_loop(0, B // 128, zero_c, 0)

    def gelu_dot(zf, rows):
        u = (zf * (0.5 + 0.5 * lax.erf(zf * SQRT_HALF))).astype(BF16)
        acc_d[...] += dot(u, bbuf[rows, :], ((0,), (0,)))

    def pass_one(s, i):
        slot = lax.rem(s, 2)
        rows = rows_of(i * R, R)

        @pl.when(i == 0)
        def _():
            acc_d[...] = jnp.zeros_like(acc_d)

        @pl.when(s < NB)
        def _():
            @pl.when(s == 0)
            def _():
                row_copy(h_hbm, abuf, asem, i).wait()
                row_copy(dy_hbm, bbuf, bsem, i).wait()

            z = dot(abuf[rows, :], wa[slot], ((1,), (0,))).astype(BF16)
            zb[rows, :] = z
            gelu_dot(z.astype(F32), rows)

        @pl.when(s >= NB)
        def _():
            for c in z_copies(s, i):
                c.wait()
            gelu_dot(zb[rows, :].astype(F32), rows)

    def slope_dot(s, rows):
        slot = lax.rem(s, 2)
        e = dot(bbuf[rows, :], wb[slot], ((1,), (1,))).astype(BF16)
        zf = zb[rows, :].astype(F32)
        slope = 0.5 + 0.5 * lax.erf(zf * SQRT_HALF) + zf * jnp.exp2(zf * zf * EXP_SCALE) * PDF_SCALE
        dd = (e.astype(F32) * slope).astype(BF16)
        acc_u[...] += dot(abuf[rows, :], dd, ((0,), (0,)))
        return dd

    def pass_two(s, i):
        slot = lax.rem(s, 2)
        rows = rows_of(i * R, R)

        @pl.when(i == 0)
        def _():
            acc_u[...] = jnp.zeros_like(acc_u)

        @pl.when(s < NB)
        def _():
            dd = slope_dot(s, rows)
            cbuf[rows, :] += dot(dd, wa[slot], ((1,), (1,)))

        @pl.when(s >= NB)
        def _():
            @pl.when(s == NB)
            def _():
                row_copy(x_hbm, abuf, asem, i).wait()

            slope_dot(s, rows)

        @pl.when(jnp.logical_and(s + 1 >= NB, s + 1 < STEPS))
        def _():
            for c in z_copies(s + 1, i):
                c.start()

    plans = (((item_d, 2, 1), (item_d, 4, 2)),
             ((item_u, 1, 1), (item_u, 3, 2), (item_u, 5, 3), (item_d, 0, 0)),
             ((item_d, 1, 0), (item_d, 3, 1), (item_d, 5, 2)),
             ((item_u, 2, 1), (item_u, 4, 2), (item_u, 0, 0)))

    def quarter(t, carry):
        s = lax.div(t, 4)
        pos = lax.rem(t, 4)
        i = lax.rem(pos, 2)

        @pl.when(t == 4 * NB)
        def _():
            for k in range(NCH):
                row_copy(x_hbm, abuf, asem, k).start()

            def conv(k, carry):
                rows = rows_of(k * 128, 128)
                bbuf[rows, :] = cbuf[rows, :].astype(BF16)
                return carry

            lax.fori_loop(0, B // 128, conv, 0)

        @pl.when(jnp.logical_and(pos == 0, s < STEPS))
        def _():
            up, down = w_copies(s)
            for c in down:
                c.wait()

            @pl.when(s < NB)
            def _():
                for c in up:
                    c.wait()

            @pl.when(s + 1 < STEPS)
            def _():
                up, down = w_copies(s + 1)
                for c in down:
                    c.start()

                @pl.when(s + 1 < NB)
                def _():
                    for c in up:
                        c.start()

        @pl.when(jnp.logical_and(pos < 2, s < STEPS))
        def _():
            pass_one(s, i)

        @pl.when(jnp.logical_and(pos >= 2, s < STEPS))
        def _():
            pass_two(s, i)

        for k, plan in enumerate(plans):
            @pl.when(pos == k)
            def _():
                tick(s, plan)
        return carry

    lax.fori_loop(0, 4 * (STEPS + 1) + 2, quarter, 0)

    for i, dev in enumerate((partner, (r + x_off, d), (r + y_off, d))):
        c = pltpu.make_async_remote_copy(src_ref=ssq.at[i], dst_ref=sq_in.at[i], send_sem=nsend.at[i],
                                         recv_sem=nrecv.at[i], device_id=dev, device_id_type=MESH)
        c.start()
        if i == 0:
            for t in range(FULL, STEPS):
                for it in (item_d, item_u):
                    for tc in tail_out(it, t):
                        tc.wait()
        c.wait()
        ssq[i + 1] = ssq[i] + sq_in[i]
    total = jnp.sum(ssq[3], axis=0, keepdims=True)
    total = jnp.sum(total, axis=1, keepdims=True)
    norm = jnp.sqrt(total)
    scale = jnp.minimum(1.0, clip_ref[0] / (norm + NORM_EPS))
    stats[0] = jnp.broadcast_to(norm, (8, 128))
    stats[1] = jnp.broadcast_to(scale, (8, 128))


def backward_reduce(clip, h, dy, x, z1, w_up, w_down):
    any_spec = pl.BlockSpec(memory_space=pl.ANY)
    vmem = pltpu.VMEM

    def item(rows, cols, acc):
        return [vmem(acc, F32), vmem((SLOTS, rows, cols), F32), vmem((SLOTS, rows // 2, cols), F32),
                vmem((SLOTS, rows // 4, cols), F32), vmem((SLOTS, rows // 2, cols), F32)]

    dma = pltpu.SemaphoreType.DMA
    return pl.pallas_call(
        mega_kernel,
        out_shape=(jax.ShapeDtypeStruct((2, NB, D // 2, BF), F32),
                   jax.ShapeDtypeStruct((2, FF // 2, D), F32),
                   jax.ShapeDtypeStruct((TAIL, 2, 192, 256), F32),
                   jax.ShapeDtypeStruct((2, 8, 128), F32)),
        in_specs=[pl.BlockSpec(memory_space=pltpu.SMEM)] + [any_spec] * 6,
        out_specs=(any_spec, any_spec, any_spec, pl.BlockSpec(memory_space=pltpu.VMEM)),
        scratch_shapes=[vmem((B, D), BF16), vmem((B, D), BF16), vmem((B, D), F32),
                        vmem((2, D, BF), BF16), vmem((2, BF, D), BF16), vmem((B, BF), BF16)]
        + item(HB, D, (BF, D)) + item(D // 2, BF, (D, BF))
        + [vmem((4, 8, 128), F32), vmem((3, 8, 128), F32)]
        + [dma((NCH,)), dma((NCH,)), dma((2, 4)), dma((NCH, 2)), dma((TAIL, 2, 3)), dma((3,)), dma((3,))]
        + [dma((5, SLOTS)), dma((5, SLOTS)), dma((SLOTS,))] * 2,
        compiler_params=pltpu.CompilerParams(collective_id=0, has_side_effects=True, vmem_limit_bytes=67043328),
        name='backward_reduce',
    )(clip, h, dy, x, z1, w_up, w_down)


def adam_rule(s, g, master_ref, mom_ref, var_ref, new_master_ref, new_mom_ref, new_var_ref, w_ref):
    mom = BETA1 * mom_ref[0] + (1.0 - BETA1) * s * g
    var = BETA2 * var_ref[0] + (1.0 - BETA2) * (s * s) * (g * g)
    master = master_ref[0] - LEARN_RATE * (mom / BIAS_ONE) / (jnp.sqrt(var / BIAS_TWO) + ADAM_EPS)
    new_mom_ref[0] = mom
    new_var_ref[0] = var
    new_master_ref[0] = master
    w_ref[0] = master.astype(BF16)


def adam_body(tail, n_alias, stats, *refs):
    s = stats[1, 0:1, 0:1]
    if tail:
        own, from_n2, from_n1, from_diag = refs[:4]
        refs = refs[4:]
        r = lax.axis_index('replica')
        d = lax.axis_index('data')
        x, y = lax.rem(r, 2), lax.div(r, 2)
        a = (1 - d) * x + d * y
        b = (1 - d) * y + d * x
        i = pl.program_id(0)
        half = lax.rem(i, 2)

        def pick(qa, qb, ty, rows):
            da = lax.rem(qa + a, 2)
            db = lax.rem(qb + b, 2)
            near = jnp.where(db == 0, own[0, ty, rows, :], from_n2[0, ty, rows, :])
            far = jnp.where(db == 0, from_n1[0, ty, rows, :], from_diag[0, ty, rows, :])
            return jnp.where(da == 0, near, far)

        up_rows = pl.ds(pl.multiple_of(half * 96, 8), 96)
        g_up = jnp.concatenate([pick(q // 2, q % 2, 1, up_rows) for q in range(4)], axis=0)
        g_down = jnp.concatenate([jnp.concatenate([pick(half, qb, 0, pl.ds(p * 64, 64)) for p in range(3)], axis=1)
                                  for qb in range(2)], axis=0)
    else:
        g_up = refs[0][0, 0]
        g_down = refs[1][0]
        refs = refs[2:]
    states, outs = refs[:6], refs[6 + n_alias:]
    adam_rule(s, g_up, *states[:3], *outs[:3], outs[6])
    adam_rule(s, g_down, *states[3:], *outs[3:6], outs[7])


def adam(stats, grads, states, prev, w, lo, hi, tail=False):
    any_spec = pl.BlockSpec(memory_space=pl.ANY)
    up = pl.BlockSpec((1, D // 2, HB), lambda i: (w, 0, lax.rem(i + lo, 2) * NB + lax.div(i + lo, 2)))
    down = pl.BlockSpec((1, 128, D), lambda i: (w, i + lo, 0))
    if tail:
        g_specs = [pl.BlockSpec((1, 2, 192, 256), lambda i: (lax.div(i, 2), 0, 0, 0))] * 4
    else:
        g_specs = [pl.BlockSpec((1, 1, D // 2, HB), lambda i: (w, lax.div(i + lo, 2), 0, lax.rem(i + lo, 2))), down]
    n = hi - lo
    full = [jax.ShapeDtypeStruct(v.shape, F32) for v in states]
    halves = [jax.ShapeDtypeStruct((n, D // 2, HB), BF16), jax.ShapeDtypeStruct((n, 128, D), BF16)]
    first = 1 + len(grads) + 6
    cells = n * (D // 2 * HB + 128 * D)
    return pl.pallas_call(
        lambda *refs: adam_body(tail, len(prev), *refs),
        grid=(n,),
        out_shape=full + halves,
        in_specs=[pl.BlockSpec((2, 8, 128), lambda i: (0, 0, 0))] + g_specs + [up] * 3 + [down] * 3 + [any_spec] * len(prev),
        out_specs=[up] * 3 + [down] * 3 + [pl.BlockSpec((1, D // 2, HB), lambda i: (i, 0, 0)), pl.BlockSpec((1, 128, D), lambda i: (i, 0, 0))],
        input_output_aliases={first + k: k for k in range(len(prev))},
        compiler_params=pltpu.CompilerParams(vmem_limit_bytes=67043328),
        cost_estimate=pl.CostEstimate(flops=cells * 400, bytes_accessed=cells * 30, transcendentals=0),
    )(stats, *grads, *states, *prev)


def place_kernel(w, lo, n, n_extra, own_u, own_d, got_u, got_d, *rest):
    out_u, out_d, buf_u, buf_d, sem_in, sem_out = rest[n_extra:]
    d = lax.axis_index('data')
    loads, stores = [], []
    for k, (src_u, src_d) in enumerate(((own_u, own_d), (got_u, got_d))):
        q = d if k == 0 else 1 - d
        loads.append(pltpu.make_async_copy(src_u, buf_u.at[k], sem_in.at[k, 0]))
        loads.append(pltpu.make_async_copy(src_d, buf_d.at[k], sem_in.at[k, 1]))
        for i in range(n):
            t = i + lo
            cols = pl.ds(((t % 2) * NB + t // 2) * HB, HB)
            stores.append((2 * k, pltpu.make_async_copy(
                buf_u.at[k, i], out_u.at[w, pl.ds(pl.multiple_of(q * (D // 2), 8), D // 2), cols], sem_out.at[k, i])))
            rows = pl.ds(pl.multiple_of(q * (FF // 2) + t * 128, 8), 128)
            stores.append((2 * k + 1, pltpu.make_async_copy(buf_d.at[k, i], out_d.at[w, rows, :], sem_out.at[k, n + i])))
    for c in loads:
        c.start()
    for k, c in enumerate(loads):
        c.wait()
        for kk, st in stores:
            if kk == k:
                st.start()
    for kk, st in stores:
        st.wait()


def place(w, lo, own, got, prev, after):
    n = own[0].shape[0]
    any_spec = pl.BlockSpec(memory_space=pl.ANY)
    extra = list(prev) + list(after)
    cells = 2 * n * (D // 2 * HB + 128 * D)
    return pl.pallas_call(
        lambda *refs: place_kernel(w, lo, n, len(extra), *refs),
        out_shape=(jax.ShapeDtypeStruct((2, D, FF), BF16), jax.ShapeDtypeStruct((2, FF, D), BF16)),
        in_specs=[any_spec] * (4 + len(extra)),
        out_specs=(any_spec, any_spec),
        scratch_shapes=[pltpu.VMEM((2, n, D // 2, HB), BF16), pltpu.VMEM((2, n, 128, D), BF16),
                        pltpu.SemaphoreType.DMA((2, 2)), pltpu.SemaphoreType.DMA((2, 2 * n))],
        input_output_aliases={4 + k: k for k in range(len(prev))},
        compiler_params=pltpu.CompilerParams(vmem_limit_bytes=67043328),
        cost_estimate=pl.CostEstimate(flops=cells * 100, bytes_accessed=cells * 4, transcendentals=0),
    )(*own, *got, *extra)


def swap(halves):
    return [lax.ppermute(v, 'data', [(0, 1), (1, 0)]) for v in halves]


def solution(mesh):
    batch_spec = P(('replica', 'data'), None)
    whole_spec = P()
    shard_spec = P(None, 'data', None)
    first_axis = [(r * 2 + d, (r ^ (1 if d == 0 else 2)) * 2 + d) for r in range(4) for d in range(2)]
    second_axis = [(r * 2 + d, (r ^ (2 if d == 0 else 1)) * 2 + d) for r in range(4) for d in range(2)]
    both_axes = [(r * 2 + d, (r ^ 3) * 2 + d) for r in range(4) for d in range(2)]

    def device_step(inp_rows, out_grad, w_up, w_down, master_up, master_down, mom_up, mom_down, var_up, var_down, clip_norm):
        pre_one = jnp.dot(inp_rows, w_up[0], preferred_element_type=F32).astype(BF16)
        act_one = gelu_value(pre_one.astype(F32)).astype(BF16)
        mid_rows = jnp.dot(act_one, w_down[0], preferred_element_type=F32).astype(BF16)
        g_up, g_down, g_tail, stats = backward_reduce(clip_norm.reshape(1), mid_rows, out_grad, inp_rows, pre_one, w_up, w_down)
        axes = ('replica', 'data')
        tails = [g_tail]
        for perm in (second_axis, first_axis, both_axes):
            tails.append(lax.ppermute(g_tail, axes, perm))
        states = [master_up, mom_up, var_up, master_down, mom_down, var_down]
        cut = 2 * (NB - TAIL)
        *new, wu, wd = adam(stats, [g_up, g_down], states, [], 1, 0, 2 * NB)
        own_a = [wu, wd]
        got_a = swap(own_a)
        *new, wu, wd = adam(stats, [g_up, g_down], states, new, 0, 0, cut)
        own_b = [wu, wd]
        got_b = swap(own_b)
        weights = place(1, 0, own_a, got_a, [], [wu])
        *new, wu, wd = adam(stats, tails, states, new, 0, cut, 2 * NB, tail=True)
        own_c = [wu, wd]
        got_c = swap(own_c)
        weights = place(0, 0, own_b, got_b, weights, [wu])
        weights = place(0, cut, own_c, got_c, weights, [])
        m_up, o_up, v_up, m_down, o_down, v_down = new
        return (weights[0], weights[1], m_up, m_down, o_up, o_down, v_up, v_down, stats[0, 0, 0])

    return jax.shard_map(device_step, mesh=mesh, in_specs=(batch_spec, batch_spec, whole_spec, whole_spec, shard_spec, shard_spec, shard_spec, shard_spec, shard_spec, shard_spec, whole_spec), out_specs=(whole_spec, whole_spec, shard_spec, shard_spec, shard_spec, shard_spec, shard_spec, shard_spec, whole_spec), check_vma=False)
```

```python
import jax
import jax.numpy as jnp
from jax import lax
from jax.experimental import pallas as pl
from jax.experimental.pallas import tpu as pltpu
from jax.sharding import PartitionSpec as P


BETA1 = 0.9
BETA2 = 0.95
ADAM_EPS = 1e-8
LEARN_RATE = 5e-3
NORM_EPS = 1e-6
STEP = 10
BIAS_ONE = 1.0 - BETA1 ** STEP
BIAS_TWO = 1.0 - BETA2 ** STEP
MESH = pl.DeviceIdType.MESH
F32 = jnp.float32
BF16 = jnp.bfloat16

B, D, FF = 4096, 768, 3072
NB = 6
HB = FF // NB // 2
BF = 2 * HB
R = B // 2
NCH = B // R
STEPS = 2 * NB
SLOTS = 3
TAIL = 3
FULL = STEPS - TAIL
SQRT_HALF = 0.7071067811865476
PDF_SCALE = 0.3989422804014327
NBUF = 2
EXP_SCALE = -0.5 * 1.4426950408889634


def gelu_value(pre_act):
    return pre_act * (0.5 + 0.5 * lax.erf(pre_act * SQRT_HALF))


def dot(a, b, dims):
    return lax.dot_general(a, b, (dims, ((), ())), preferred_element_type=F32)


class Item:
    def __init__(self, rows, cols, refs, sems):
        self.rows, self.cols = rows, cols
        self.acc, self.r0, self.r1, self.r2, self.hh = refs
        self.send, self.recv, self.loc = sems


def mega_kernel(clip_ref, h_hbm, dy_hbm, x_hbm, z_hbm, wu_hbm, wd_hbm,
                gup, gdn, gtail, stats,
                abuf, bbuf, cbuf, wa, wb, zb,
                acc_d, r0_d, r1_d, r2_d, h_d,
                acc_u, r0_u, r1_u, r2_u, h_u,
                ssq, sq_in, asem, bsem, wsem, zsem, tsem, nsend, nrecv,
                send_d, recv_d, loc_d, send_u, recv_u, loc_u):
    r = lax.axis_index('replica')
    d = lax.axis_index('data')
    x = lax.rem(r, 2)
    y = lax.div(r, 2)
    x_off = 1 - 2 * x
    y_off = 2 - 4 * y
    partner = (r, 1 - d)
    n1 = (r + (1 - d) * x_off + d * y_off, d)
    n2 = (r + (1 - d) * y_off + d * x_off, d)
    a = (1 - d) * x + d * y
    b = (1 - d) * y + d * x

    item_d = Item(HB, D, (acc_d, r0_d, r1_d, r2_d, h_d), (send_d, recv_d, loc_d))
    item_u = Item(D // 2, BF, (acc_u, r0_u, r1_u, r2_u, h_u), (send_u, recv_u, loc_u))

    def rows_of(start, size):
        return pl.ds(pl.multiple_of(start, 8), size)

    def row_copy(src, dst, sem, i):
        rows = rows_of(i * R, R)
        return pltpu.make_async_copy(src.at[rows, :], dst.at[rows, :], sem.at[i])

    def w_copies(s):
        slot = lax.rem(s, 2)
        j = lax.rem(s, NB)
        ph = 1 - lax.div(s, NB)
        up, down = [], []
        for p in range(2):
            cols = pl.ds(pl.multiple_of(p * (FF // 2) + j * HB, 128), HB)
            up.append(pltpu.make_async_copy(wu_hbm.at[1, :, cols], wa.at[slot, :, p * HB:(p + 1) * HB], wsem.at[slot, p]))
            down.append(pltpu.make_async_copy(wd_hbm.at[ph, cols, :], wb.at[slot, p * HB:(p + 1) * HB, :], wsem.at[slot, 2 + p]))
        return up, down

    def z_copies(s, i):
        j = lax.rem(s, NB)
        out = []
        for p in range(2):
            cols = pl.ds(pl.multiple_of(p * (FF // 2) + j * HB, 128), HB)
            rows = rows_of(i * R, R)
            out.append(pltpu.make_async_copy(z_hbm.at[rows, cols], zb.at[rows, p * HB:(p + 1) * HB], zsem.at[i, p]))
        return out

    def g_rows(it, s, part, size):
        w = 1 - lax.div(s, NB)
        j = lax.rem(s, NB)
        if it is item_d:
            return gdn.at[w, rows_of(j * HB + part, size), :]
        return gup.at[w, j, rows_of(part, size), :]

    def cp(it, stage, s):
        k = lax.rem(s, SLOTS)
        rows = it.rows
        half, quarter = rows // 2, rows // 4
        if stage == 0:
            src, dst, dev = it.acc.at[rows_of((1 - d) * rows, rows), :], it.r0.at[k], partner
        elif stage == 1:
            src, dst, dev = it.r0.at[k, rows_of((1 - a) * half, half), :], it.r1.at[k], n1
        elif stage == 2:
            src, dst, dev = it.r1.at[k, rows_of((1 - b) * quarter, quarter), :], it.r2.at[k], n2
        elif stage == 3:
            q = rows_of(b * quarter, quarter)
            src, dst, dev = it.hh.at[k, q, :], it.hh.at[k, q, :], n2
        else:
            src, dst, dev = it.hh.at[k], g_rows(it, s, a * half, half), n1
        return pltpu.make_async_remote_copy(src_ref=src, dst_ref=dst, send_sem=it.send.at[stage, k],
                                            recv_sem=it.recv.at[stage, k], device_id=dev, device_id_type=MESH)

    def local_out(it, s):
        k = lax.rem(s, SLOTS)
        half = it.rows // 2
        return pltpu.make_async_copy(it.hh.at[k], g_rows(it, s, a * half, half), it.loc.at[k])

    def fold(it, stage, s):
        k = lax.rem(s, SLOTS)
        rows = it.rows
        half, quarter = rows // 2, rows // 4
        if stage == 0:
            return
        cp(it, stage - 1, s).wait()
        if stage == 1:
            it.r0[k] = it.r0[k] + it.acc[rows_of(d * rows, rows), :]
        elif stage == 2:
            it.r1[k] = it.r1[k] + it.r0[k, rows_of(a * half, half), :]
        elif stage == 3:
            g = (it.r2[k] + it.r1[k, rows_of(b * quarter, quarter), :]) * 0.125
            it.hh[k, rows_of(b * quarter, quarter), :] = g
            sq = g * g
            sq = sq.reshape(quarter // 8, 8, it.cols).sum(axis=0)
            tot = sq[:, :128]
            for c in range(1, it.cols // 128):
                tot = tot + sq[:, c * 128:(c + 1) * 128]
            ssq[0] += tot
        elif stage == 5:
            local_out(it, s).wait()

    def tail_out(it, s):
        k = lax.rem(s, SLOTS)
        quarter = it.rows // 4
        ty = 0 if it is item_d else 1
        return [pltpu.make_async_copy(it.hh.at[k, rows_of(b * quarter, quarter), p * 256:(p + 1) * 256],
                                      gtail.at[s - FULL, ty, p * quarter:(p + 1) * quarter, :],
                                      tsem.at[s - FULL, ty, p]) for p in range(it.cols // 256)]

    def post(it, stage, s):
        if stage == 3:
            @pl.when(s < FULL)
            def _():
                cp(it, 3, s).start()

            @pl.when(s >= FULL)
            def _():
                for c in tail_out(it, s):
                    c.start()
        elif stage < 5:
            cp(it, stage, s).start()
        if stage == 4:
            local_out(it, s).start()

    def tick(s, plan):
        late = None
        for it, stage, lag in plan:
            t = s - lag
            ok = jnp.logical_and(t >= 0, t < (FULL if stage >= 4 else STEPS))

            @pl.when(ok)
            def _():
                fold(it, stage, t)

            if late is not None:
                pit, pstage, pt, pok = late

                @pl.when(pok)
                def _():
                    post(pit, pstage, pt)
            late = (it, stage, t, ok)
        pit, pstage, pt, pok = late

        @pl.when(pok)
        def _():
            post(pit, pstage, pt)

    ssq[0] = jnp.zeros((8, 128), F32)
    for i in range(NCH):
        row_copy(h_hbm, abuf, asem, i).start()
        row_copy(dy_hbm, bbuf, bsem, i).start()
        if i == 0:
            up, down = w_copies(0)
            for c in up + down:
                c.start()

    barrier = pltpu.get_barrier_semaphore()
    for dev in (partner, n1, n2):
        pl.semaphore_signal(barrier, inc=1, device_id=dev, device_id_type=MESH)
    pl.semaphore_wait(barrier, 3)

    def zero_c(i, carry):
        cbuf[rows_of(i * 128, 128), :] = jnp.zeros((128, D), F32)
        return carry

    lax.fori_loop(0, B // 128, zero_c, 0)

    def gelu_dot(zf, rows):
        u = (zf * (0.5 + 0.5 * lax.erf(zf * SQRT_HALF))).astype(BF16)
        acc_d[...] += dot(u, bbuf[rows, :], ((0,), (0,)))

    def pass_one(s, i):
        slot = lax.rem(s, 2)
        rows = rows_of(i * R, R)

        @pl.when(i == 0)
        def _():
            acc_d[...] = jnp.zeros_like(acc_d)

        @pl.when(s < NB)
        def _():
            @pl.when(s == 0)
            def _():
                row_copy(h_hbm, abuf, asem, i).wait()
                row_copy(dy_hbm, bbuf, bsem, i).wait()

            z = dot(abuf[rows, :], wa[slot], ((1,), (0,))).astype(BF16)
            zb[rows, :] = z
            gelu_dot(z.astype(F32), rows)

        @pl.when(s >= NB)
        def _():
            for c in z_copies(s, i):
                c.wait()
            gelu_dot(zb[rows, :].astype(F32), rows)

    def slope_dot(s, rows):
        slot = lax.rem(s, 2)
        e = dot(bbuf[rows, :], wb[slot], ((1,), (1,))).astype(BF16)
        zf = zb[rows, :].astype(F32)
        slope = 0.5 + 0.5 * lax.erf(zf * SQRT_HALF) + zf * jnp.exp2(zf * zf * EXP_SCALE) * PDF_SCALE
        dd = (e.astype(F32) * slope).astype(BF16)
        acc_u[...] += dot(abuf[rows, :], dd, ((0,), (0,)))
        return dd

    def pass_two(s, i):
        slot = lax.rem(s, 2)
        rows = rows_of(i * R, R)

        @pl.when(i == 0)
        def _():
            acc_u[...] = jnp.zeros_like(acc_u)

        @pl.when(s < NB)
        def _():
            dd = slope_dot(s, rows)
            cbuf[rows, :] += dot(dd, wa[slot], ((1,), (1,)))

        @pl.when(s >= NB)
        def _():
            @pl.when(s == NB)
            def _():
                row_copy(x_hbm, abuf, asem, i).wait()

            slope_dot(s, rows)

        @pl.when(jnp.logical_and(s + 1 >= NB, s + 1 < STEPS))
        def _():
            for c in z_copies(s + 1, i):
                c.start()

    plans = (((item_d, 2, 1), (item_d, 4, 2)),
             ((item_u, 1, 1), (item_u, 3, 2), (item_u, 5, 3), (item_d, 0, 0)),
             ((item_d, 1, 0), (item_d, 3, 1), (item_d, 5, 2)),
             ((item_u, 2, 1), (item_u, 4, 2), (item_u, 0, 0)))

    def quarter(t, carry):
        s = lax.div(t, 4)
        pos = lax.rem(t, 4)
        i = lax.rem(pos, 2)

        @pl.when(t == 4 * NB)
        def _():
            for k in range(NCH):
                row_copy(x_hbm, abuf, asem, k).start()

            def conv(k, carry):
                rows = rows_of(k * 128, 128)
                bbuf[rows, :] = cbuf[rows, :].astype(BF16)
                return carry

            lax.fori_loop(0, B // 128, conv, 0)

        @pl.when(jnp.logical_and(pos == 0, s < STEPS))
        def _():
            up, down = w_copies(s)
            for c in down:
                c.wait()

            @pl.when(s < NB)
            def _():
                for c in up:
                    c.wait()

            @pl.when(s + 1 < STEPS)
            def _():
                up, down = w_copies(s + 1)
                for c in down:
                    c.start()

                @pl.when(s + 1 < NB)
                def _():
                    for c in up:
                        c.start()

        @pl.when(jnp.logical_and(pos < 2, s < STEPS))
        def _():
            pass_one(s, i)

        @pl.when(jnp.logical_and(pos >= 2, s < STEPS))
        def _():
            pass_two(s, i)

        for k, plan in enumerate(plans):
            @pl.when(pos == k)
            def _():
                tick(s, plan)
        return carry

    lax.fori_loop(0, 4 * (STEPS + 1) + 2, quarter, 0)

    for i, dev in enumerate((partner, (r + x_off, d), (r + y_off, d))):
        c = pltpu.make_async_remote_copy(src_ref=ssq.at[i], dst_ref=sq_in.at[i], send_sem=nsend.at[i],
                                         recv_sem=nrecv.at[i], device_id=dev, device_id_type=MESH)
        c.start()
        if i == 0:
            for t in range(FULL, STEPS):
                for it in (item_d, item_u):
                    for tc in tail_out(it, t):
                        tc.wait()
        c.wait()
        ssq[i + 1] = ssq[i] + sq_in[i]
    total = jnp.sum(ssq[3], axis=0, keepdims=True)
    total = jnp.sum(total, axis=1, keepdims=True)
    norm = jnp.sqrt(total)
    scale = jnp.minimum(1.0, clip_ref[0] / (norm + NORM_EPS))
    stats[0] = jnp.broadcast_to(norm, (8, 128))
    stats[1] = jnp.broadcast_to(scale, (8, 128))


def backward_reduce(clip, h, dy, x, z1, w_up, w_down):
    any_spec = pl.BlockSpec(memory_space=pl.ANY)
    vmem = pltpu.VMEM

    def item(rows, cols, acc):
        return [vmem(acc, F32), vmem((SLOTS, rows, cols), F32), vmem((SLOTS, rows // 2, cols), F32),
                vmem((SLOTS, rows // 4, cols), F32), vmem((SLOTS, rows // 2, cols), F32)]

    dma = pltpu.SemaphoreType.DMA
    return pl.pallas_call(
        mega_kernel,
        out_shape=(jax.ShapeDtypeStruct((2, NB, D // 2, BF), F32),
                   jax.ShapeDtypeStruct((2, FF // 2, D), F32),
                   jax.ShapeDtypeStruct((TAIL, 2, 192, 256), F32),
                   jax.ShapeDtypeStruct((2, 8, 128), F32)),
        in_specs=[pl.BlockSpec(memory_space=pltpu.SMEM)] + [any_spec] * 6,
        out_specs=(any_spec, any_spec, any_spec, pl.BlockSpec(memory_space=pltpu.VMEM)),
        scratch_shapes=[vmem((B, D), BF16), vmem((B, D), BF16), vmem((B, D), F32),
                        vmem((2, D, BF), BF16), vmem((2, BF, D), BF16), vmem((B, BF), BF16)]
        + item(HB, D, (BF, D)) + item(D // 2, BF, (D, BF))
        + [vmem((4, 8, 128), F32), vmem((3, 8, 128), F32)]
        + [dma((NCH,)), dma((NCH,)), dma((2, 4)), dma((NCH, 2)), dma((TAIL, 2, 3)), dma((3,)), dma((3,))]
        + [dma((5, SLOTS)), dma((5, SLOTS)), dma((SLOTS,))] * 2,
        compiler_params=pltpu.CompilerParams(collective_id=0, has_side_effects=True, vmem_limit_bytes=67043328),
        name='backward_reduce',
    )(clip, h, dy, x, z1, w_up, w_down)


def forward_body(x, wu, wd, z_ref, h_ref):
    z = dot(x[...], wu[0], ((1,), (0,))).astype(BF16)
    z_ref[...] = z
    u = gelu_value(z.astype(F32)).astype(BF16)
    h_ref[...] = dot(u, wd[0], ((1,), (0,))).astype(BF16)


def forward(x, w_up, w_down):
    rows = 1024
    once = pl.Buffered(1)
    return pl.pallas_call(
        forward_body,
        grid=(B // rows,),
        out_shape=(jax.ShapeDtypeStruct((B, FF), BF16), jax.ShapeDtypeStruct((B, D), BF16)),
        in_specs=[pl.BlockSpec((rows, D), lambda i: (i, 0)),
                  pl.BlockSpec((1, D, FF), lambda i: (0, 0, 0), pipeline_mode=once),
                  pl.BlockSpec((1, FF, D), lambda i: (0, 0, 0), pipeline_mode=once)],
        out_specs=(pl.BlockSpec((rows, FF), lambda i: (i, 0)), pl.BlockSpec((rows, D), lambda i: (i, 0))),
        compiler_params=pltpu.CompilerParams(vmem_limit_bytes=67043328),
        name='forward',
    )(x, w_up, w_down)


def adam_rule(s, g, master_ref, mom_ref, var_ref, new_master_ref, new_mom_ref, new_var_ref, w_refs):
    mom = BETA1 * mom_ref[0] + (1.0 - BETA1) * s * g
    var = BETA2 * var_ref[0] + (1.0 - BETA2) * (s * s) * (g * g)
    master = master_ref[0] - LEARN_RATE * (mom / BIAS_ONE) / (jnp.sqrt(var / BIAS_TWO) + ADAM_EPS)
    new_mom_ref[0] = mom
    new_var_ref[0] = var
    new_master_ref[0] = master
    w = master.astype(BF16)
    for ref in w_refs:
        ref[0] = w


def adam_body(tail, n_alias, me, stats, *refs):
    s = stats[1, 0:1, 0:1]
    if tail:
        own, from_n2, from_n1, from_diag = refs[:4]
        refs = refs[4:]
        r = lax.axis_index('replica')
        d = lax.axis_index('data')
        x, y = lax.rem(r, 2), lax.div(r, 2)
        a = (1 - d) * x + d * y
        b = (1 - d) * y + d * x
        i = pl.program_id(0)
        half = lax.rem(i, 2)

        def pick(qa, qb, ty, rows):
            da = lax.rem(qa + a, 2)
            db = lax.rem(qb + b, 2)
            near = jnp.where(db == 0, own[0, ty, rows, :], from_n2[0, ty, rows, :])
            far = jnp.where(db == 0, from_n1[0, ty, rows, :], from_diag[0, ty, rows, :])
            return jnp.where(da == 0, near, far)

        up_rows = pl.ds(pl.multiple_of(half * 96, 8), 96)
        g_up = jnp.concatenate([pick(q // 2, q % 2, 1, up_rows) for q in range(4)], axis=0)
        g_down = jnp.concatenate([jnp.concatenate([pick(half, qb, 0, pl.ds(p * 64, 64)) for p in range(3)], axis=1)
                                  for qb in range(2)], axis=0)
    else:
        g_up = refs[0][0, 0]
        g_down = refs[1][0]
        refs = refs[2:]
    states, outs = refs[:6], refs[6 + n_alias:]
    adam_rule(s, g_up, *states[:3], *outs[:3], (outs[6], outs[8]))
    adam_rule(s, g_down, *states[3:], *outs[3:6], (outs[7], outs[9]))


def adam(me, stats, grads, states, prev, w, lo, hi, tail=False):
    any_spec = pl.BlockSpec(memory_space=pl.ANY)
    deep = pl.Buffered(NBUF)

    def col(i):
        return lax.rem(i + lo, 2) * NB + lax.div(i + lo, 2)

    def specs(**kw):
        up = pl.BlockSpec((1, D // 2, HB), lambda i, me: (w, 0, col(i)), **kw)
        down = pl.BlockSpec((1, 128, D), lambda i, me: (w, i + lo, 0), **kw)
        return [up] * 3 + [down] * 3

    if tail:
        g_specs = [pl.BlockSpec((1, 2, 192, 256), lambda i, me: (lax.div(i, 2), 0, 0, 0))] * 4
    else:
        g_specs = [pl.BlockSpec((1, 1, D // 2, HB), lambda i, me: (w, lax.div(i + lo, 2), 0, lax.rem(i + lo, 2)), pipeline_mode=deep),
                   pl.BlockSpec((1, 128, D), lambda i, me: (w, i + lo, 0), pipeline_mode=deep)]
    n = hi - lo
    full = [jax.ShapeDtypeStruct(v.shape, F32) for v in states]
    whole = [jax.ShapeDtypeStruct((2, D, FF), BF16), jax.ShapeDtypeStruct((2, FF, D), BF16)]
    halves = [jax.ShapeDtypeStruct((n, D // 2, HB), BF16), jax.ShapeDtypeStruct((n, 128, D), BF16)]
    first = 2 + len(grads) + 6
    cells = n * (D // 2 * HB + 128 * D)
    return pl.pallas_call(
        lambda *refs: adam_body(tail, len(prev), *refs),
        out_shape=full + whole + halves,
        grid_spec=pltpu.PrefetchScalarGridSpec(
            num_scalar_prefetch=1,
            grid=(n,),
            in_specs=[pl.BlockSpec((2, 8, 128), lambda i, me: (0, 0, 0))] + g_specs + specs(pipeline_mode=deep) + [any_spec] * len(prev),
            out_specs=specs() + [pl.BlockSpec((1, D // 2, HB), lambda i, me: (w, me[0], col(i))),
                                 pl.BlockSpec((1, 128, D), lambda i, me: (w, me[0] * (FF // 256) + i + lo, 0)),
                                 pl.BlockSpec((1, D // 2, HB), lambda i, me: (i, 0, 0)),
                                 pl.BlockSpec((1, 128, D), lambda i, me: (i, 0, 0))]),
        input_output_aliases={first + k: k for k in range(len(prev))},
        compiler_params=pltpu.CompilerParams(vmem_limit_bytes=67043328),
        cost_estimate=pl.CostEstimate(flops=cells * 400, bytes_accessed=cells * 30, transcendentals=0),
    )(me, stats, *grads, *states, *prev)


def place_kernel(w, lo, n, n_extra, got_u, got_d, *rest):
    out_u, out_d, buf_u, buf_d, sem_in, sem_out = rest[n_extra:]
    q = 1 - lax.axis_index('data')
    loads = [pltpu.make_async_copy(got_u, buf_u, sem_in.at[0]), pltpu.make_async_copy(got_d, buf_d, sem_in.at[1])]
    stores = []
    for i in range(n):
        t = i + lo
        cols = pl.ds(((t % 2) * NB + t // 2) * HB, HB)
        stores.append((0, pltpu.make_async_copy(
            buf_u.at[i], out_u.at[w, pl.ds(pl.multiple_of(q * (D // 2), 8), D // 2), cols], sem_out.at[i])))
        rows = pl.ds(pl.multiple_of(q * (FF // 2) + t * 128, 8), 128)
        stores.append((1, pltpu.make_async_copy(buf_d.at[i], out_d.at[w, rows, :], sem_out.at[n + i])))
    for c in loads:
        c.start()
    for k, c in enumerate(loads):
        c.wait()
        for kk, st in stores:
            if kk == k:
                st.start()
    for kk, st in stores:
        st.wait()


def place(w, lo, got, weights, after):
    n = got[0].shape[0]
    any_spec = pl.BlockSpec(memory_space=pl.ANY)
    extra = list(weights) + list(after)
    cells = n * (D // 2 * HB + 128 * D)
    return pl.pallas_call(
        lambda *refs: place_kernel(w, lo, n, len(extra), *refs),
        out_shape=(jax.ShapeDtypeStruct((2, D, FF), BF16), jax.ShapeDtypeStruct((2, FF, D), BF16)),
        in_specs=[any_spec] * (2 + len(extra)),
        out_specs=(any_spec, any_spec),
        scratch_shapes=[pltpu.VMEM((n, D // 2, HB), BF16), pltpu.VMEM((n, 128, D), BF16),
                        pltpu.SemaphoreType.DMA((2,)), pltpu.SemaphoreType.DMA((2 * n,))],
        input_output_aliases={2 + k: k for k in range(2)},
        compiler_params=pltpu.CompilerParams(vmem_limit_bytes=67043328),
        cost_estimate=pl.CostEstimate(flops=cells * 100, bytes_accessed=cells * 4, transcendentals=0),
    )(*got, *extra)


def swap(halves):
    return [lax.ppermute(v, 'data', [(0, 1), (1, 0)]) for v in halves]


def solution(mesh):
    batch_spec = P(('replica', 'data'), None)
    whole_spec = P()
    shard_spec = P(None, 'data', None)
    first_axis = [(r * 2 + d, (r ^ (1 if d == 0 else 2)) * 2 + d) for r in range(4) for d in range(2)]
    second_axis = [(r * 2 + d, (r ^ (2 if d == 0 else 1)) * 2 + d) for r in range(4) for d in range(2)]
    both_axes = [(r * 2 + d, (r ^ 3) * 2 + d) for r in range(4) for d in range(2)]

    def device_step(inp_rows, out_grad, w_up, w_down, master_up, master_down, mom_up, mom_down, var_up, var_down, clip_norm):
        pre_one, mid_rows = forward(inp_rows, w_up, w_down)
        g_up, g_down, g_tail, stats = backward_reduce(clip_norm.reshape(1), mid_rows, out_grad, inp_rows, pre_one, w_up, w_down)
        axes = ('replica', 'data')
        tails = [g_tail]
        for perm in (second_axis, first_axis, both_axes):
            tails.append(lax.ppermute(g_tail, axes, perm))
        states = [master_up, mom_up, var_up, master_down, mom_down, var_down]
        cut = 2 * (NB - TAIL)
        me = lax.axis_index('data').astype(jnp.int32).reshape(1)
        *new, wu, wd = adam(me, stats, [g_up, g_down], states, [], 1, 0, 2 * NB)
        got_a = swap([wu, wd])
        *new, wu, wd = adam(me, stats, [g_up, g_down], states, new, 0, 0, cut)
        got_b = swap([wu, wd])
        new[6:] = place(1, 0, got_a, new[6:], [])
        *new, wu, wd = adam(me, stats, tails, states, new, 0, cut, 2 * NB, tail=True)
        got_c = swap([wu, wd])
        new[6:] = place(0, 0, got_b, new[6:], [])
        new[6:] = place(0, cut, got_c, new[6:], [])
        m_up, o_up, v_up, m_down, o_down, v_down, new_up, new_down = new
        return (new_up, new_down, m_up, m_down, o_up, o_down, v_up, v_down, stats[0, 0, 0])

    return jax.shard_map(device_step, mesh=mesh, in_specs=(batch_spec, batch_spec, whole_spec, whole_spec, shard_spec, shard_spec, shard_spec, shard_spec, shard_spec, shard_spec, whole_spec), out_specs=(whole_spec, whole_spec, shard_spec, shard_spec, shard_spec, shard_spec, shard_spec, shard_spec, whole_spec), check_vma=False)
```

```python
import jax
import jax.numpy as jnp
from jax import lax
from jax.experimental import pallas as pl
from jax.experimental.pallas import tpu as pltpu
from jax.sharding import PartitionSpec as P


BETA1 = 0.9
BETA2 = 0.95
ADAM_EPS = 1e-8
LEARN_RATE = 5e-3
NORM_EPS = 1e-6
STEP = 10
BIAS_ONE = 1.0 - BETA1 ** STEP
BIAS_TWO = 1.0 - BETA2 ** STEP
MESH = pl.DeviceIdType.MESH
F32 = jnp.float32
BF16 = jnp.bfloat16

B, D, FF = 4096, 768, 3072
NB = 6
HB = FF // NB // 2
BF = 2 * HB
R = B // 2
NCH = B // R
STEPS = 2 * NB
SLOTS = 3
TAIL = 3
FULL = STEPS - TAIL
SQRT_HALF = 0.7071067811865476
PDF_SCALE = 0.3989422804014327
NBUF = 4
EXP_SCALE = -0.5 * 1.4426950408889634


def gelu_value(pre_act):
    return pre_act * (0.5 + 0.5 * lax.erf(pre_act * SQRT_HALF))


def dot(a, b, dims):
    return lax.dot_general(a, b, (dims, ((), ())), preferred_element_type=F32)


class Item:
    def __init__(self, rows, cols, refs, sems):
        self.rows, self.cols = rows, cols
        self.acc, self.r0, self.r1, self.r2, self.hh = refs
        self.send, self.recv, self.loc = sems


def mega_kernel(clip_ref, h_hbm, dy_hbm, x_hbm, z_hbm, wu_hbm, wd_hbm,
                gup, gdn, gtail, stats,
                abuf, bbuf, cbuf, wa, wb, zb,
                acc_d, r0_d, r1_d, r2_d, h_d,
                acc_u, r0_u, r1_u, r2_u, h_u,
                ssq, sq_in, asem, bsem, wsem, zsem, tsem, nsend, nrecv,
                send_d, recv_d, loc_d, send_u, recv_u, loc_u):
    r = lax.axis_index('replica')
    d = lax.axis_index('data')
    x = lax.rem(r, 2)
    y = lax.div(r, 2)
    x_off = 1 - 2 * x
    y_off = 2 - 4 * y
    partner = (r, 1 - d)
    n1 = (r + (1 - d) * x_off + d * y_off, d)
    n2 = (r + (1 - d) * y_off + d * x_off, d)
    a = (1 - d) * x + d * y
    b = (1 - d) * y + d * x

    item_d = Item(HB, D, (acc_d, r0_d, r1_d, r2_d, h_d), (send_d, recv_d, loc_d))
    item_u = Item(D // 2, BF, (acc_u, r0_u, r1_u, r2_u, h_u), (send_u, recv_u, loc_u))

    def rows_of(start, size):
        return pl.ds(pl.multiple_of(start, 8), size)

    def row_copy(src, dst, sem, i):
        rows = rows_of(i * R, R)
        return pltpu.make_async_copy(src.at[rows, :], dst.at[rows, :], sem.at[i])

    def w_copies(s):
        slot = lax.rem(s, 2)
        j = lax.rem(s, NB)
        ph = 1 - lax.div(s, NB)
        up, down = [], []
        for p in range(2):
            cols = pl.ds(pl.multiple_of(p * (FF // 2) + j * HB, 128), HB)
            up.append(pltpu.make_async_copy(wu_hbm.at[1, :, cols], wa.at[slot, :, p * HB:(p + 1) * HB], wsem.at[slot, p]))
            down.append(pltpu.make_async_copy(wd_hbm.at[ph, cols, :], wb.at[slot, p * HB:(p + 1) * HB, :], wsem.at[slot, 2 + p]))
        return up, down

    def z_copies(s, i):
        j = lax.rem(s, NB)
        out = []
        for p in range(2):
            cols = pl.ds(pl.multiple_of(p * (FF // 2) + j * HB, 128), HB)
            rows = rows_of(i * R, R)
            out.append(pltpu.make_async_copy(z_hbm.at[rows, cols], zb.at[rows, p * HB:(p + 1) * HB], zsem.at[i, p]))
        return out

    def g_rows(it, s, part, size):
        w = 1 - lax.div(s, NB)
        j = lax.rem(s, NB)
        if it is item_d:
            return gdn.at[w, rows_of(j * HB + part, size), :]
        return gup.at[w, j, rows_of(part, size), :]

    def cp(it, stage, s):
        k = lax.rem(s, SLOTS)
        rows = it.rows
        half, quarter = rows // 2, rows // 4
        if stage == 0:
            src, dst, dev = it.acc.at[rows_of((1 - d) * rows, rows), :], it.r0.at[k], partner
        elif stage == 1:
            src, dst, dev = it.r0.at[k, rows_of((1 - a) * half, half), :], it.r1.at[k], n1
        elif stage == 2:
            src, dst, dev = it.r1.at[k, rows_of((1 - b) * quarter, quarter), :], it.r2.at[k], n2
        elif stage == 3:
            q = rows_of(b * quarter, quarter)
            src, dst, dev = it.hh.at[k, q, :], it.hh.at[k, q, :], n2
        else:
            src, dst, dev = it.hh.at[k], g_rows(it, s, a * half, half), n1
        return pltpu.make_async_remote_copy(src_ref=src, dst_ref=dst, send_sem=it.send.at[stage, k],
                                            recv_sem=it.recv.at[stage, k], device_id=dev, device_id_type=MESH)

    def local_out(it, s):
        k = lax.rem(s, SLOTS)
        half = it.rows // 2
        return pltpu.make_async_copy(it.hh.at[k], g_rows(it, s, a * half, half), it.loc.at[k])

    def fold(it, stage, s):
        k = lax.rem(s, SLOTS)
        rows = it.rows
        half, quarter = rows // 2, rows // 4
        if stage == 0:
            return
        cp(it, stage - 1, s).wait()
        if stage == 1:
            it.r0[k] = it.r0[k] + it.acc[rows_of(d * rows, rows), :]
        elif stage == 2:
            it.r1[k] = it.r1[k] + it.r0[k, rows_of(a * half, half), :]
        elif stage == 3:
            g = (it.r2[k] + it.r1[k, rows_of(b * quarter, quarter), :]) * 0.125
            it.hh[k, rows_of(b * quarter, quarter), :] = g
            sq = g * g
            sq = sq.reshape(quarter // 8, 8, it.cols).sum(axis=0)
            tot = sq[:, :128]
            for c in range(1, it.cols // 128):
                tot = tot + sq[:, c * 128:(c + 1) * 128]
            ssq[0] += tot
        elif stage == 5:
            local_out(it, s).wait()

    def tail_out(it, s):
        k = lax.rem(s, SLOTS)
        quarter = it.rows // 4
        ty = 0 if it is item_d else 1
        return [pltpu.make_async_copy(it.hh.at[k, rows_of(b * quarter, quarter), p * 256:(p + 1) * 256],
                                      gtail.at[s - FULL, ty, p * quarter:(p + 1) * quarter, :],
                                      tsem.at[s - FULL, ty, p]) for p in range(it.cols // 256)]

    def post(it, stage, s):
        if stage == 3:
            @pl.when(s < FULL)
            def _():
                cp(it, 3, s).start()

            @pl.when(s >= FULL)
            def _():
                for c in tail_out(it, s):
                    c.start()
        elif stage < 5:
            cp(it, stage, s).start()
        if stage == 4:
            local_out(it, s).start()

    def tick(s, plan):
        late = None
        for it, stage, lag in plan:
            t = s - lag
            ok = jnp.logical_and(t >= 0, t < (FULL if stage >= 4 else STEPS))

            @pl.when(ok)
            def _():
                fold(it, stage, t)

            if late is not None:
                pit, pstage, pt, pok = late

                @pl.when(pok)
                def _():
                    post(pit, pstage, pt)
            late = (it, stage, t, ok)
        pit, pstage, pt, pok = late

        @pl.when(pok)
        def _():
            post(pit, pstage, pt)

    ssq[0] = jnp.zeros((8, 128), F32)
    up, down = w_copies(0)
    for c in [row_copy(h_hbm, abuf, asem, 0)] + up + [row_copy(dy_hbm, bbuf, bsem, 0)] + down:
        c.start()

    barrier = pltpu.get_barrier_semaphore()
    for fy in range(2):
        for fx in range(2):
            for fd in range(2):
                if fy + fx + fd:
                    dev = (2 * (y + fy - 2 * fy * y) + x + fx - 2 * fx * x, d + fd - 2 * fd * d)
                    pl.semaphore_signal(barrier, inc=1, device_id=dev, device_id_type=MESH)
    pl.semaphore_wait(barrier, 7)

    def zero_c(i, carry):
        cbuf[rows_of(i * 128, 128), :] = jnp.zeros((128, D), F32)
        return carry

    lax.fori_loop(0, B // 128, zero_c, 0)

    def gelu_dot(zf, rows):
        u = (zf * (0.5 + 0.5 * lax.erf(zf * SQRT_HALF))).astype(BF16)
        acc_d[...] += dot(u, bbuf[rows, :], ((0,), (0,)))

    def pass_one(s, i):
        slot = lax.rem(s, 2)
        rows = rows_of(i * R, R)

        @pl.when(i == 0)
        def _():
            acc_d[...] = jnp.zeros_like(acc_d)

        @pl.when(s < NB)
        def _():
            @pl.when(s == 0)
            def _():
                row_copy(h_hbm, abuf, asem, i).wait()
                row_copy(dy_hbm, bbuf, bsem, i).wait()

                @pl.when(i + 1 < NCH)
                def _():
                    row_copy(h_hbm, abuf, asem, i + 1).start()
                    row_copy(dy_hbm, bbuf, bsem, i + 1).start()

            z = dot(abuf[rows, :], wa[slot], ((1,), (0,))).astype(BF16)
            zb[rows, :] = z
            gelu_dot(z.astype(F32), rows)

        @pl.when(s >= NB)
        def _():
            for c in z_copies(s, i):
                c.wait()
            gelu_dot(zb[rows, :].astype(F32), rows)

    def slope_dot(s, rows):
        slot = lax.rem(s, 2)
        e = dot(bbuf[rows, :], wb[slot], ((1,), (1,))).astype(BF16)
        zf = zb[rows, :].astype(F32)
        slope = 0.5 + 0.5 * lax.erf(zf * SQRT_HALF) + zf * jnp.exp2(zf * zf * EXP_SCALE) * PDF_SCALE
        dd = (e.astype(F32) * slope).astype(BF16)
        acc_u[...] += dot(abuf[rows, :], dd, ((0,), (0,)))
        return dd

    def pass_two(s, i):
        slot = lax.rem(s, 2)
        rows = rows_of(i * R, R)

        @pl.when(i == 0)
        def _():
            acc_u[...] = jnp.zeros_like(acc_u)

        @pl.when(s < NB)
        def _():
            dd = slope_dot(s, rows)
            cbuf[rows, :] += dot(dd, wa[slot], ((1,), (1,)))

        @pl.when(s >= NB)
        def _():
            @pl.when(s == NB)
            def _():
                row_copy(x_hbm, abuf, asem, i).wait()

            slope_dot(s, rows)

        @pl.when(jnp.logical_and(s + 1 >= NB, s + 1 < STEPS))
        def _():
            for c in z_copies(s + 1, i):
                c.start()

    plans = (((item_d, 2, 1), (item_d, 4, 2)),
             ((item_u, 1, 1), (item_u, 3, 2), (item_u, 5, 3), (item_d, 0, 0)),
             ((item_d, 1, 0), (item_d, 3, 1), (item_d, 5, 2)),
             ((item_u, 2, 1), (item_u, 4, 2), (item_u, 0, 0)))

    def quarter(t, carry):
        s = lax.div(t, 4)
        pos = lax.rem(t, 4)
        i = lax.rem(pos, 2)

        @pl.when(t == 4 * NB)
        def _():
            for k in range(NCH):
                row_copy(x_hbm, abuf, asem, k).start()

            def conv(k, carry):
                rows = rows_of(k * 128, 128)
                bbuf[rows, :] = cbuf[rows, :].astype(BF16)
                return carry

            lax.fori_loop(0, B // 128, conv, 0)

        @pl.when(jnp.logical_and(pos == 0, s < STEPS))
        def _():
            up, down = w_copies(s)
            for c in down:
                c.wait()

            @pl.when(s < NB)
            def _():
                for c in up:
                    c.wait()

            @pl.when(s + 1 < STEPS)
            def _():
                up, down = w_copies(s + 1)
                for c in down:
                    c.start()

                @pl.when(s + 1 < NB)
                def _():
                    for c in up:
                        c.start()

        @pl.when(jnp.logical_and(pos < 2, s < STEPS))
        def _():
            pass_one(s, i)

        @pl.when(jnp.logical_and(pos >= 2, s < STEPS))
        def _():
            pass_two(s, i)

        for k, plan in enumerate(plans):
            @pl.when(pos == k)
            def _():
                tick(s, plan)
        return carry

    lax.fori_loop(0, 4 * (STEPS + 1) + 2, quarter, 0)

    peers = [(2 * (y + fy - 2 * fy * y) + x + fx - 2 * fx * x, d + fd - 2 * fd * d)
             for fy in range(2) for fx in range(2) for fd in range(2)]
    sq_in[0] = ssq[0]
    for t in range(FULL, STEPS):
        for it in (item_d, item_u):
            for tc in tail_out(it, t):
                tc.wait()
    exchange = [pltpu.make_async_remote_copy(src_ref=ssq.at[0], dst_ref=sq_in.at[k], send_sem=nsend.at[k],
                                             recv_sem=nrecv.at[k], device_id=peers[k], device_id_type=MESH)
                for k in range(1, 8)]
    for c in exchange:
        c.start()
    for c in exchange:
        c.wait()
    total = jnp.zeros((8, 128), F32)
    for iy in range(2):
        for ix in range(2):
            for dd in range(2):
                total = total + sq_in[4 * lax.rem(iy + y, 2) + 2 * lax.rem(ix + x, 2) + lax.rem(dd + d, 2)]
    total = jnp.sum(total, axis=0, keepdims=True)
    total = jnp.sum(total, axis=1, keepdims=True)
    norm = jnp.sqrt(total)
    scale = jnp.minimum(1.0, clip_ref[0] / (norm + NORM_EPS))
    stats[0] = jnp.broadcast_to(norm, (8, 128))
    stats[1] = jnp.broadcast_to(scale, (8, 128))


def backward_reduce(clip, h, dy, x, z1, w_up, w_down):
    any_spec = pl.BlockSpec(memory_space=pl.ANY)
    vmem = pltpu.VMEM

    def item(rows, cols, acc):
        return [vmem(acc, F32), vmem((SLOTS, rows, cols), F32), vmem((SLOTS, rows // 2, cols), F32),
                vmem((SLOTS, rows // 4, cols), F32), vmem((SLOTS, rows // 2, cols), F32)]

    dma = pltpu.SemaphoreType.DMA
    return pl.pallas_call(
        mega_kernel,
        out_shape=(jax.ShapeDtypeStruct((2, NB, D // 2, BF), F32),
                   jax.ShapeDtypeStruct((2, FF // 2, D), F32),
                   jax.ShapeDtypeStruct((TAIL, 2, 192, 256), F32),
                   jax.ShapeDtypeStruct((2, 8, 128), F32)),
        in_specs=[pl.BlockSpec(memory_space=pltpu.SMEM)] + [any_spec] * 6,
        out_specs=(any_spec, any_spec, any_spec, pl.BlockSpec(memory_space=pltpu.VMEM)),
        scratch_shapes=[vmem((B, D), BF16), vmem((B, D), BF16), vmem((B, D), F32),
                        vmem((2, D, BF), BF16), vmem((2, BF, D), BF16), vmem((B, BF), BF16)]
        + item(HB, D, (BF, D)) + item(D // 2, BF, (D, BF))
        + [vmem((1, 8, 128), F32), vmem((8, 8, 128), F32)]
        + [dma((NCH,)), dma((NCH,)), dma((2, 4)), dma((NCH, 2)), dma((TAIL, 2, 3)), dma((8,)), dma((8,))]
        + [dma((5, SLOTS)), dma((5, SLOTS)), dma((SLOTS,))] * 2,
        compiler_params=pltpu.CompilerParams(collective_id=0, has_side_effects=True, vmem_limit_bytes=67043328),
        name='backward_reduce',
    )(clip, h, dy, x, z1, w_up, w_down)


def forward_body(x, wu, wd, z_ref, h_ref):
    z = dot(x[...], wu[0], ((1,), (0,))).astype(BF16)
    z_ref[...] = z
    u = gelu_value(z.astype(F32)).astype(BF16)
    h_ref[...] = dot(u, wd[0], ((1,), (0,))).astype(BF16)


def forward(x, w_up, w_down):
    rows = 1024
    once = pl.Buffered(1)
    return pl.pallas_call(
        forward_body,
        grid=(B // rows,),
        out_shape=(jax.ShapeDtypeStruct((B, FF), BF16), jax.ShapeDtypeStruct((B, D), BF16)),
        in_specs=[pl.BlockSpec((rows, D), lambda i: (i, 0)),
                  pl.BlockSpec((1, D, FF), lambda i: (0, 0, 0), pipeline_mode=once),
                  pl.BlockSpec((1, FF, D), lambda i: (0, 0, 0), pipeline_mode=once)],
        out_specs=(pl.BlockSpec((rows, FF), lambda i: (i, 0)), pl.BlockSpec((rows, D), lambda i: (i, 0))),
        compiler_params=pltpu.CompilerParams(vmem_limit_bytes=67043328),
        name='forward',
    )(x, w_up, w_down)


def adam_rule(s, g, master, mom, var):
    mom = BETA1 * mom + (1.0 - BETA1) * s * g
    var = BETA2 * var + (1.0 - BETA2) * (s * s) * (g * g)
    master = master - LEARN_RATE * (mom / BIAS_ONE) / (jnp.sqrt(var / BIAS_TWO) + ADAM_EPS)
    return master, mom, var


def adam_kernel(w, j0, nj, tail, n_alias, stats, *refs):
    n = 2 * nj
    ru = D // 2 // n
    n_grads = 4 if tail else 2
    grads, refs = refs[:n_grads], refs[n_grads:]
    states, refs = refs[:6], refs[6 + n_alias:]
    outs, refs = refs[:10], refs[10:]
    if not n_alias:
        norm_out, refs = refs[0], refs[1:]
        norm_out[0] = jnp.max(stats[0])
    in_u, in_d, g_u, g_d, out_u, out_d, w_u, w_d, gt, isem, osem, gsem = refs
    d = lax.axis_index('data')
    s = stats[1, 0:1, 0:1]

    def up_at(ref, p, row0, size):
        return ref.at[w, pl.ds(pl.multiple_of(row0, 8), size), pl.ds((p * NB + j0) * HB, nj * HB)]

    def loads(i):
        k = lax.rem(i, NBUF)
        row = pl.ds(pl.multiple_of((i + 2 * j0) * 128, 8), 128)
        cs = []
        if not tail:
            rows = pl.ds(pl.multiple_of(i * ru, 8), ru)
            cs.append(pltpu.make_async_copy(grads[0].at[w, pl.ds(j0, nj), rows, :], g_u.at[k], isem.at[k, 9]))
            cs.append(pltpu.make_async_copy(grads[1].at[w, row, :], g_d.at[k], isem.at[k, 10]))
        for q in range(3):
            for p in range(2):
                cs.append(pltpu.make_async_copy(up_at(states[q], p, i * ru, ru), in_u.at[k, q, p], isem.at[k, 2 * q + p]))
            cs.append(pltpu.make_async_copy(states[3 + q].at[w, row, :], in_d.at[k, q], isem.at[k, 6 + q]))
        return cs

    def stores(i):
        k = lax.rem(i, 2)
        row = pl.ds(pl.multiple_of((i + 2 * j0) * 128, 8), 128)
        cs = []
        for q in range(3):
            for p in range(2):
                cs.append(pltpu.make_async_copy(out_u.at[k, q, p], up_at(outs[q], p, i * ru, ru), osem.at[k, 2 * q + p]))
            cs.append(pltpu.make_async_copy(out_d.at[k, q], outs[3 + q].at[w, row, :], osem.at[k, 6 + q]))
        for p in range(2):
            cs.append(pltpu.make_async_copy(w_u.at[k, p], up_at(outs[6], p, d * (D // 2) + i * ru, ru), osem.at[k, 9 + p]))
        my_down = pl.ds(pl.multiple_of(d * (FF // 2) + (i + 2 * j0) * 128, 8), 128)
        cs.append(pltpu.make_async_copy(w_d.at[k], outs[7].at[w, my_down, :], osem.at[k, 11]))
        cs.append(pltpu.make_async_copy(w_u.at[k], outs[8].at[:, pl.ds(pl.multiple_of(i * ru, 8), ru), :], osem.at[k, 12]))
        cs.append(pltpu.make_async_copy(w_d.at[k], outs[9].at[i], osem.at[k, 13]))
        return cs

    for i in range(NBUF):
        for c in loads(i):
            c.start()
    if tail:
        g_loads = [pltpu.make_async_copy(grads[q], gt.at[q], gsem.at[q]) for q in range(4)]
        for c in g_loads:
            c.start()
        for c in g_loads:
            c.wait()
        r = lax.axis_index('replica')
        x, y = lax.rem(r, 2), lax.div(r, 2)
        a = (1 - d) * x + d * y
        b = (1 - d) * y + d * x

    def block(i, carry):
        k = lax.rem(i, NBUF)
        o = lax.rem(i, 2)
        for c in loads(i):
            c.wait()

        @pl.when(i >= 2)
        def _():
            for c in stores(i - 2):
                c.wait()

        for t in range(ru // 32):
            rows = slice(t * 32, (t + 1) * 32)
            if tail:
                third = i * (ru // 32) + t
                quarter = lax.div(third, 3)
                src = 2 * lax.rem(lax.div(quarter, 2) + a, 2) + lax.rem(lax.rem(quarter, 2) + b, 2)
                g_row = lax.rem(third, 3) * 32
            for p in range(2):
                for j in range(nj):
                    cols = slice(j * HB, (j + 1) * HB)
                    if tail:
                        g = gt[src, j, 1, pl.ds(pl.multiple_of(p * 96 + g_row, 8), 32), :]
                    else:
                        g = g_u[k, j, rows, p * HB:(p + 1) * HB]
                    res = adam_rule(s, g, in_u[k, 0, p, rows, cols], in_u[k, 1, p, rows, cols], in_u[k, 2, p, rows, cols])
                    for q in range(3):
                        out_u[o, q, p, rows, cols] = res[q]
                    w_u[o, p, rows, cols] = res[0].astype(BF16)
        for t in range(8):
            rows = slice(t * 16, (t + 1) * 16)
            if tail:
                half = lax.rem(i, 2)
                src = 2 * lax.rem(half + a, 2) + lax.rem(t // 4 + b, 2)
                g = jnp.concatenate([gt[src, lax.div(i, 2), 0, p * 64 + (t % 4) * 16:p * 64 + (t % 4) * 16 + 16, :] for p in range(3)], axis=1)
            else:
                g = g_d[k, rows, :]
            res = adam_rule(s, g, in_d[k, 0, rows, :], in_d[k, 1, rows, :], in_d[k, 2, rows, :])
            for q in range(3):
                out_d[o, q, rows, :] = res[q]
            w_d[o, rows, :] = res[0].astype(BF16)
        for c in stores(i):
            c.start()

        @pl.when(i + NBUF < n)
        def _():
            for c in loads(i + NBUF):
                c.start()

        return carry

    lax.fori_loop(0, n, block, 0)
    for i in (n - 2, n - 1):
        for c in stores(i):
            c.wait()


def adam(stats, grads, states, prev, w, j0, nj, tail=False):
    any_spec = pl.BlockSpec(memory_space=pl.ANY)
    n = 2 * nj
    ru = D // 2 // n
    full = [jax.ShapeDtypeStruct(v.shape, F32) for v in states]
    whole = [jax.ShapeDtypeStruct((2, D, FF), BF16), jax.ShapeDtypeStruct((2, FF, D), BF16)]
    halves = [jax.ShapeDtypeStruct((2, D // 2, nj * HB), BF16), jax.ShapeDtypeStruct((n, 128, D), BF16)]
    norm = [] if prev else [jax.ShapeDtypeStruct((1,), F32)]
    first = 1 + len(grads) + 6
    cells = D * nj * HB * 2
    vmem, dma = pltpu.VMEM, pltpu.SemaphoreType.DMA
    return pl.pallas_call(
        lambda *refs: adam_kernel(w, j0, nj, tail, len(prev), *refs),
        out_shape=full + whole + halves + norm,
        in_specs=[pl.BlockSpec(memory_space=pltpu.VMEM)] + [any_spec] * (len(grads) + 6 + len(prev)),
        out_specs=[any_spec] * 10 + [pl.BlockSpec(memory_space=pltpu.SMEM)] * len(norm),
        scratch_shapes=[vmem((NBUF, 3, 2, ru, nj * HB), F32), vmem((NBUF, 3, 128, D), F32),
                        vmem((NBUF, nj, ru, BF), F32), vmem((NBUF, 128, D), F32),
                        vmem((2, 3, 2, ru, nj * HB), F32), vmem((2, 3, 128, D), F32),
                        vmem((2, 2, ru, nj * HB), BF16), vmem((2, 128, D), BF16),
                        vmem((4, TAIL, 2, 192, 256), F32), dma((NBUF, 11)), dma((2, 14)), dma((4,))],
        input_output_aliases={first + k: k for k in range(len(prev))},
        compiler_params=pltpu.CompilerParams(vmem_limit_bytes=67043328),
        cost_estimate=pl.CostEstimate(flops=cells * 400, bytes_accessed=cells * 30, transcendentals=0),
    )(stats, *grads, *states, *prev)


def place_kernel(w, j0, nj, got_u, got_d, _u, _d, out_u, out_d, buf_u, buf_d, sem_in, sem_out):
    q = 1 - lax.axis_index('data')
    rows = pl.ds(pl.multiple_of(q * (D // 2), 8), D // 2)
    loads, stores = [], []
    for p in range(2):
        loads.append(pltpu.make_async_copy(got_u.at[p], buf_u.at[p], sem_in.at[p]))
        stores.append(pltpu.make_async_copy(buf_u.at[p], out_u.at[w, rows, pl.ds((p * NB + j0) * HB, nj * HB)], sem_out.at[p]))
    for p in range(2):
        part = pl.ds(p * nj, nj)
        loads.append(pltpu.make_async_copy(got_d.at[part], buf_d.at[part], sem_in.at[2 + p]))
        for i in range(nj):
            t = p * nj + i
            to = pl.ds(pl.multiple_of(q * (FF // 2) + (t + 2 * j0) * 128, 8), 128)
            stores.append(pltpu.make_async_copy(buf_d.at[t], out_d.at[w, to, :], sem_out.at[2 + t]))
    for c in loads:
        c.start()
    for k, c in enumerate(loads):
        c.wait()
        for st in stores[k:k + 1] if k < 2 else stores[2 + (k - 2) * nj:2 + (k - 1) * nj]:
            st.start()
    for st in stores:
        st.wait()


def place(w, j0, nj, got, weights):
    any_spec = pl.BlockSpec(memory_space=pl.ANY)
    n = 2 * nj
    cells = D * nj * HB * 2
    return pl.pallas_call(
        lambda *refs: place_kernel(w, j0, nj, *refs),
        out_shape=(jax.ShapeDtypeStruct((2, D, FF), BF16), jax.ShapeDtypeStruct((2, FF, D), BF16)),
        in_specs=[any_spec] * 4,
        out_specs=(any_spec, any_spec),
        scratch_shapes=[pltpu.VMEM((2, D // 2, nj * HB), BF16), pltpu.VMEM((n, 128, D), BF16),
                        pltpu.SemaphoreType.DMA((4,)), pltpu.SemaphoreType.DMA((2 + n,))],
        input_output_aliases={2 + k: k for k in range(2)},
        compiler_params=pltpu.CompilerParams(vmem_limit_bytes=67043328),
        cost_estimate=pl.CostEstimate(flops=cells * 100, bytes_accessed=cells * 4, transcendentals=0),
    )(*got, *weights)


def swap(halves):
    return [lax.ppermute(v, 'data', [(0, 1), (1, 0)]) for v in halves]


def solution(mesh):
    batch_spec = P(('replica', 'data'), None)
    whole_spec = P()
    shard_spec = P(None, 'data', None)
    first_axis = [(r * 2 + d, (r ^ (1 if d == 0 else 2)) * 2 + d) for r in range(4) for d in range(2)]
    second_axis = [(r * 2 + d, (r ^ (2 if d == 0 else 1)) * 2 + d) for r in range(4) for d in range(2)]

    def device_step(inp_rows, out_grad, w_up, w_down, master_up, master_down, mom_up, mom_down, var_up, var_down, clip_norm):
        pre_one, mid_rows = forward(inp_rows, w_up, w_down)
        g_up, g_down, g_tail, stats = backward_reduce(clip_norm.reshape(1), mid_rows, out_grad, inp_rows, pre_one, w_up, w_down)
        axes = ('replica', 'data')
        tails = [g_tail]
        for perm in (second_axis, first_axis):
            tails.append(lax.ppermute(g_tail, axes, perm))
        tails.append(lax.ppermute(tails[1], axes, first_axis))
        states = [master_up, mom_up, var_up, master_down, mom_down, var_down]
        cut = NB - TAIL
        *new, wu, wd, norm = adam(stats, [g_up, g_down], states, [], 1, 0, NB)
        got_a = swap([wu, wd])
        *new, wu, wd = adam(stats, [g_up, g_down], states, new, 0, 0, cut)
        got_b = swap([wu, wd])
        new[6:] = place(1, 0, NB, got_a, new[6:])
        *new, wu, wd = adam(stats, tails, states, new, 0, cut, TAIL, tail=True)
        got_c = swap([wu, wd])
        new[6:] = place(0, 0, cut, got_b, new[6:])
        new[6:] = place(0, cut, TAIL, got_c, new[6:])
        m_up, o_up, v_up, m_down, o_down, v_down, new_up, new_down = new
        return (new_up, new_down, m_up, m_down, o_up, o_down, v_up, v_down, norm.reshape(()))

    return jax.shard_map(device_step, mesh=mesh, in_specs=(batch_spec, batch_spec, whole_spec, whole_spec, shard_spec, shard_spec, shard_spec, shard_spec, shard_spec, shard_spec, whole_spec), out_specs=(whole_spec, whole_spec, shard_spec, shard_spec, shard_spec, shard_spec, shard_spec, shard_spec, whole_spec), check_vma=False)
```

```python
import jax
import jax.numpy as jnp
from jax import lax
from jax.experimental import pallas as pl
from jax.experimental.pallas import tpu as pltpu
from jax.sharding import PartitionSpec as P


BETA1 = 0.9
BETA2 = 0.95
ADAM_EPS = 1e-8
LEARN_RATE = 5e-3
NORM_EPS = 1e-6
STEP = 10
BIAS_ONE = 1.0 - BETA1 ** STEP
BIAS_TWO = 1.0 - BETA2 ** STEP
MESH = pl.DeviceIdType.MESH
F32 = jnp.float32
BF16 = jnp.bfloat16

B, D, FF = 4096, 768, 3072
NB = 6
HB = FF // NB // 2
BF = 2 * HB
R = B // 2
NCH = B // R
STEPS = 2 * NB
SLOTS = 3
TAIL = 3
FULL = STEPS - TAIL
SQRT_HALF = 0.7071067811865476
PDF_SCALE = 0.3989422804014327
NBUF = 4
EXP_SCALE = -0.5 * 1.4426950408889634


def gelu_value(pre_act):
    return pre_act * (0.5 + 0.5 * lax.erf(pre_act * SQRT_HALF))


def dot(a, b, dims):
    return lax.dot_general(a, b, (dims, ((), ())), preferred_element_type=F32)


class Item:
    def __init__(self, rows, cols, refs, sems):
        self.rows, self.cols = rows, cols
        self.acc, self.r0, self.r1, self.r2, self.hh = refs
        self.send, self.recv, self.loc = sems


def mega_kernel(clip_ref, h_hbm, dy_hbm, x_hbm, z_hbm, wu_hbm, wd_hbm,
                gup, gdn, gtail, stats,
                abuf, bbuf, cbuf, wa, wb, zb,
                acc_d, r0_d, r1_d, r2_d, h_d,
                acc_u, r0_u, r1_u, r2_u, h_u,
                ssq, sq_in, asem, bsem, wsem, zsem, tsem, nsend, nrecv,
                send_d, recv_d, loc_d, send_u, recv_u, loc_u):
    r = lax.axis_index('replica')
    d = lax.axis_index('data')
    x = lax.rem(r, 2)
    y = lax.div(r, 2)
    x_off = 1 - 2 * x
    y_off = 2 - 4 * y
    partner = (r, 1 - d)
    n1 = (r + (1 - d) * x_off + d * y_off, d)
    n2 = (r + (1 - d) * y_off + d * x_off, d)
    a = (1 - d) * x + d * y
    b = (1 - d) * y + d * x

    item_d = Item(HB, D, (acc_d, r0_d, r1_d, r2_d, h_d), (send_d, recv_d, loc_d))
    item_u = Item(D // 2, BF, (acc_u, r0_u, r1_u, r2_u, h_u), (send_u, recv_u, loc_u))

    def rows_of(start, size):
        return pl.ds(pl.multiple_of(start, 8), size)

    def row_copy(src, dst, sem, i):
        rows = rows_of(i * R, R)
        return pltpu.make_async_copy(src.at[rows, :], dst.at[rows, :], sem.at[i])

    def w_copies(s):
        slot = lax.rem(s, 2)
        j = lax.rem(s, NB)
        ph = 1 - lax.div(s, NB)
        up, down = [], []
        for p in range(2):
            cols = pl.ds(pl.multiple_of(p * (FF // 2) + j * HB, 128), HB)
            up.append(pltpu.make_async_copy(wu_hbm.at[1, :, cols], wa.at[slot, :, p * HB:(p + 1) * HB], wsem.at[slot, p]))
            down.append(pltpu.make_async_copy(wd_hbm.at[ph, cols, :], wb.at[slot, p * HB:(p + 1) * HB, :], wsem.at[slot, 2 + p]))
        return up, down

    def z_copies(s, i):
        j = lax.rem(s, NB)
        out = []
        for p in range(2):
            cols = pl.ds(pl.multiple_of(p * (FF // 2) + j * HB, 128), HB)
            rows = rows_of(i * R, R)
            out.append(pltpu.make_async_copy(z_hbm.at[rows, cols], zb.at[rows, p * HB:(p + 1) * HB], zsem.at[i, p]))
        return out

    def g_rows(it, s, part, size):
        w = 1 - lax.div(s, NB)
        j = lax.rem(s, NB)
        if it is item_d:
            return gdn.at[w, rows_of(j * HB + part, size), :]
        return gup.at[w, j, rows_of(part, size), :]

    def cp(it, stage, s):
        k = lax.rem(s, SLOTS)
        rows = it.rows
        half, quarter = rows // 2, rows // 4
        if stage == 0:
            src, dst, dev = it.acc.at[rows_of((1 - d) * rows, rows), :], it.r0.at[k], partner
        elif stage == 1:
            src, dst, dev = it.r0.at[k, rows_of((1 - a) * half, half), :], it.r1.at[k], n1
        elif stage == 2:
            src, dst, dev = it.r1.at[k, rows_of((1 - b) * quarter, quarter), :], it.r2.at[k], n2
        elif stage == 3:
            q = rows_of(b * quarter, quarter)
            src, dst, dev = it.hh.at[k, q, :], it.hh.at[k, q, :], n2
        else:
            src, dst, dev = it.hh.at[k], g_rows(it, s, a * half, half), n1
        return pltpu.make_async_remote_copy(src_ref=src, dst_ref=dst, send_sem=it.send.at[stage, k],
                                            recv_sem=it.recv.at[stage, k], device_id=dev, device_id_type=MESH)

    def local_out(it, s):
        k = lax.rem(s, SLOTS)
        half = it.rows // 2
        return pltpu.make_async_copy(it.hh.at[k], g_rows(it, s, a * half, half), it.loc.at[k])

    def fold(it, stage, s):
        k = lax.rem(s, SLOTS)
        rows = it.rows
        half, quarter = rows // 2, rows // 4
        if stage == 0:
            return
        cp(it, stage - 1, s).wait()
        if stage == 1:
            it.r0[k] = it.r0[k] + it.acc[rows_of(d * rows, rows), :]
        elif stage == 2:
            it.r1[k] = it.r1[k] + it.r0[k, rows_of(a * half, half), :]
        elif stage == 3:
            g = (it.r2[k] + it.r1[k, rows_of(b * quarter, quarter), :]) * 0.125
            it.hh[k, rows_of(b * quarter, quarter), :] = g
            sq = g * g
            sq = sq.reshape(quarter // 8, 8, it.cols).sum(axis=0)
            tot = sq[:, :128]
            for c in range(1, it.cols // 128):
                tot = tot + sq[:, c * 128:(c + 1) * 128]
            ssq[0] += tot
        elif stage == 5:
            local_out(it, s).wait()

    def tail_out(it, s):
        k = lax.rem(s, SLOTS)
        quarter = it.rows // 4
        ty = 0 if it is item_d else 1
        return [pltpu.make_async_copy(it.hh.at[k, rows_of(b * quarter, quarter), p * 256:(p + 1) * 256],
                                      gtail.at[s - FULL, ty, p * quarter:(p + 1) * quarter, :],
                                      tsem.at[s - FULL, ty, p]) for p in range(it.cols // 256)]

    def post(it, stage, s):
        if stage == 3:
            @pl.when(s < FULL)
            def _():
                cp(it, 3, s).start()

            @pl.when(s >= FULL)
            def _():
                for c in tail_out(it, s):
                    c.start()
        elif stage < 5:
            cp(it, stage, s).start()
        if stage == 4:
            local_out(it, s).start()

    def tick(s, plan):
        late = None
        for it, stage, lag in plan:
            t = s - lag
            ok = jnp.logical_and(t >= 0, t < (FULL if stage >= 4 else STEPS))

            @pl.when(ok)
            def _():
                fold(it, stage, t)

            if late is not None:
                pit, pstage, pt, pok = late

                @pl.when(pok)
                def _():
                    post(pit, pstage, pt)
            late = (it, stage, t, ok)
        pit, pstage, pt, pok = late

        @pl.when(pok)
        def _():
            post(pit, pstage, pt)

    ssq[0] = jnp.zeros((8, 128), F32)
    up, down = w_copies(0)
    for c in [row_copy(h_hbm, abuf, asem, 0)] + up + [row_copy(dy_hbm, bbuf, bsem, 0)] + down:
        c.start()

    barrier = pltpu.get_barrier_semaphore()
    for fy in range(2):
        for fx in range(2):
            for fd in range(2):
                if fy + fx + fd:
                    dev = (2 * (y + fy - 2 * fy * y) + x + fx - 2 * fx * x, d + fd - 2 * fd * d)
                    pl.semaphore_signal(barrier, inc=1, device_id=dev, device_id_type=MESH)
    pl.semaphore_wait(barrier, 7)

    def zero_c(i, carry):
        cbuf[rows_of(i * 128, 128), :] = jnp.zeros((128, D), F32)
        return carry

    lax.fori_loop(0, B // 128, zero_c, 0)

    def gelu_dot(zf, rows, i):
        u = (zf * (0.5 + 0.5 * lax.erf(zf * SQRT_HALF))).astype(BF16)
        acc_d[...] = jnp.where(i == 0, 0.0, acc_d[...]) + dot(u, bbuf[rows, :], ((0,), (0,)))

    def pass_one(s, i):
        slot = lax.rem(s, 2)
        rows = rows_of(i * R, R)

        @pl.when(s < NB)
        def _():
            @pl.when(s == 0)
            def _():
                row_copy(h_hbm, abuf, asem, i).wait()
                row_copy(dy_hbm, bbuf, bsem, i).wait()

                @pl.when(i + 1 < NCH)
                def _():
                    row_copy(h_hbm, abuf, asem, i + 1).start()
                    row_copy(dy_hbm, bbuf, bsem, i + 1).start()

            z = dot(abuf[rows, :], wa[slot], ((1,), (0,))).astype(BF16)
            zb[rows, :] = z
            gelu_dot(z.astype(F32), rows, i)

        @pl.when(s >= NB)
        def _():
            for c in z_copies(s, i):
                c.wait()
            gelu_dot(zb[rows, :].astype(F32), rows, i)

    def slope_dot(s, rows, i):
        slot = lax.rem(s, 2)
        e = dot(bbuf[rows, :], wb[slot], ((1,), (1,))).astype(BF16)
        zf = zb[rows, :].astype(F32)
        slope = 0.5 + 0.5 * lax.erf(zf * SQRT_HALF) + zf * jnp.exp2(zf * zf * EXP_SCALE) * PDF_SCALE
        dd = (e.astype(F32) * slope).astype(BF16)
        acc_u[...] = jnp.where(i == 0, 0.0, acc_u[...]) + dot(abuf[rows, :], dd, ((0,), (0,)))
        return dd

    def pass_two(s, i):
        slot = lax.rem(s, 2)
        rows = rows_of(i * R, R)

        @pl.when(s < NB)
        def _():
            dd = slope_dot(s, rows, i)
            cbuf[rows, :] += dot(dd, wa[slot], ((1,), (1,)))

        @pl.when(s >= NB)
        def _():
            @pl.when(s == NB)
            def _():
                row_copy(x_hbm, abuf, asem, i).wait()

            slope_dot(s, rows, i)

        @pl.when(jnp.logical_and(s + 1 >= NB, s + 1 < STEPS))
        def _():
            for c in z_copies(s + 1, i):
                c.start()

    plans = (((item_u, 1, 1), (item_d, 4, 2)),
             ((item_d, 2, 1), (item_u, 3, 2), (item_d, 0, 0)),
             ((item_d, 1, 0), (item_d, 3, 1), (item_u, 5, 3)),
             ((item_u, 2, 1), (item_u, 4, 2), (item_d, 5, 2), (item_u, 0, 0)))

    def quarter(t, carry):
        s = lax.div(t, 4)
        pos = lax.rem(t, 4)
        i = lax.rem(pos, 2)

        @pl.when(t == 4 * NB)
        def _():
            for k in range(NCH):
                row_copy(x_hbm, abuf, asem, k).start()

            def conv(k, carry):
                rows = rows_of(k * 128, 128)
                bbuf[rows, :] = cbuf[rows, :].astype(BF16)
                return carry

            lax.fori_loop(0, B // 128, conv, 0)

        @pl.when(jnp.logical_and(pos == 0, s < STEPS))
        def _():
            up, down = w_copies(s)
            for c in down:
                c.wait()

            @pl.when(s < NB)
            def _():
                for c in up:
                    c.wait()

            @pl.when(s + 1 < STEPS)
            def _():
                up, down = w_copies(s + 1)
                for c in down:
                    c.start()

                @pl.when(s + 1 < NB)
                def _():
                    for c in up:
                        c.start()

        @pl.when(jnp.logical_and(pos < 2, s < STEPS))
        def _():
            pass_one(s, i)

        @pl.when(jnp.logical_and(pos >= 2, s < STEPS))
        def _():
            pass_two(s, i)

        for k, plan in enumerate(plans):
            @pl.when(pos == k)
            def _():
                tick(s, plan)
        return carry

    lax.fori_loop(0, 4 * (STEPS + 1) + 2, quarter, 0)

    peers = [(2 * (y + fy - 2 * fy * y) + x + fx - 2 * fx * x, d + fd - 2 * fd * d)
             for fy in range(2) for fx in range(2) for fd in range(2)]
    sq_in[0] = ssq[0]
    for t in range(FULL, STEPS):
        for it in (item_d, item_u):
            for tc in tail_out(it, t):
                tc.wait()
    exchange = [pltpu.make_async_remote_copy(src_ref=ssq.at[0], dst_ref=sq_in.at[k], send_sem=nsend.at[k],
                                             recv_sem=nrecv.at[k], device_id=peers[k], device_id_type=MESH)
                for k in range(1, 8)]
    for c in exchange:
        c.start()
    for c in exchange:
        c.wait()
    total = jnp.zeros((8, 128), F32)
    for iy in range(2):
        for ix in range(2):
            for dd in range(2):
                total = total + sq_in[4 * lax.rem(iy + y, 2) + 2 * lax.rem(ix + x, 2) + lax.rem(dd + d, 2)]
    total = jnp.sum(total, axis=0, keepdims=True)
    total = jnp.sum(total, axis=1, keepdims=True)
    norm = jnp.sqrt(total)
    scale = jnp.minimum(1.0, clip_ref[0] / (norm + NORM_EPS))
    stats[0] = jnp.broadcast_to(norm, (8, 128))
    stats[1] = jnp.broadcast_to(scale, (8, 128))


def backward_reduce(clip, h, dy, x, z1, w_up, w_down):
    any_spec = pl.BlockSpec(memory_space=pl.ANY)
    vmem = pltpu.VMEM

    def item(rows, cols, acc):
        return [vmem(acc, F32), vmem((SLOTS, rows, cols), F32), vmem((SLOTS, rows // 2, cols), F32),
                vmem((SLOTS, rows // 4, cols), F32), vmem((SLOTS, rows // 2, cols), F32)]

    dma = pltpu.SemaphoreType.DMA
    return pl.pallas_call(
        mega_kernel,
        out_shape=(jax.ShapeDtypeStruct((2, NB, D // 2, BF), F32),
                   jax.ShapeDtypeStruct((2, FF // 2, D), F32),
                   jax.ShapeDtypeStruct((TAIL, 2, 192, 256), F32),
                   jax.ShapeDtypeStruct((2, 8, 128), F32)),
        in_specs=[pl.BlockSpec(memory_space=pltpu.SMEM)] + [any_spec] * 6,
        out_specs=(any_spec, any_spec, any_spec, pl.BlockSpec(memory_space=pltpu.VMEM)),
        scratch_shapes=[vmem((B, D), BF16), vmem((B, D), BF16), vmem((B, D), F32),
                        vmem((2, D, BF), BF16), vmem((2, BF, D), BF16), vmem((B, BF), BF16)]
        + item(HB, D, (BF, D)) + item(D // 2, BF, (D, BF))
        + [vmem((1, 8, 128), F32), vmem((8, 8, 128), F32)]
        + [dma((NCH,)), dma((NCH,)), dma((2, 4)), dma((NCH, 2)), dma((TAIL, 2, 3)), dma((8,)), dma((8,))]
        + [dma((5, SLOTS)), dma((5, SLOTS)), dma((SLOTS,))] * 2,
        compiler_params=pltpu.CompilerParams(collective_id=0, has_side_effects=True, vmem_limit_bytes=67043328),
        name='backward_reduce',
    )(clip, h, dy, x, z1, w_up, w_down)


def forward_body(x, wu, wd, z_ref, h_ref):
    z = dot(x[...], wu[0], ((1,), (0,))).astype(BF16)
    z_ref[...] = z
    u = gelu_value(z.astype(F32)).astype(BF16)
    h_ref[...] = dot(u, wd[0], ((1,), (0,))).astype(BF16)


def forward(x, w_up, w_down):
    rows = 1024
    once = pl.Buffered(1)
    return pl.pallas_call(
        forward_body,
        grid=(B // rows,),
        out_shape=(jax.ShapeDtypeStruct((B, FF), BF16), jax.ShapeDtypeStruct((B, D), BF16)),
        in_specs=[pl.BlockSpec((rows, D), lambda i: (i, 0)),
                  pl.BlockSpec((1, D, FF), lambda i: (0, 0, 0), pipeline_mode=once),
                  pl.BlockSpec((1, FF, D), lambda i: (0, 0, 0), pipeline_mode=once)],
        out_specs=(pl.BlockSpec((rows, FF), lambda i: (i, 0)), pl.BlockSpec((rows, D), lambda i: (i, 0))),
        compiler_params=pltpu.CompilerParams(vmem_limit_bytes=67043328),
        name='forward',
    )(x, w_up, w_down)


def adam_rule(s, g, master, mom, var):
    mom = BETA1 * mom + (1.0 - BETA1) * s * g
    var = BETA2 * var + (1.0 - BETA2) * (s * s) * (g * g)
    master = master - LEARN_RATE * (mom / BIAS_ONE) / (jnp.sqrt(var / BIAS_TWO) + ADAM_EPS)
    return master, mom, var


def adam_kernel(w, j0, nj, tail, n_alias, stats, *refs):
    n = 2 * nj
    ru = D // 2 // n
    n_grads = 4 if tail else 2
    grads, refs = refs[:n_grads], refs[n_grads:]
    states, refs = refs[:6], refs[6 + n_alias:]
    outs, refs = refs[:10], refs[10:]
    if not n_alias:
        norm_out, refs = refs[0], refs[1:]
        norm_out[0] = jnp.max(stats[0])
    in_u, in_d, g_u, g_d, out_u, out_d, w_u, w_d, gt, isem, osem, gsem = refs
    d = lax.axis_index('data')
    s = stats[1, 0:1, 0:1]

    def up_at(ref, p, row0, size):
        return ref.at[w, pl.ds(pl.multiple_of(row0, 8), size), pl.ds((p * NB + j0) * HB, nj * HB)]

    def loads(i):
        k = lax.rem(i, NBUF)
        row = pl.ds(pl.multiple_of((i + 2 * j0) * 128, 8), 128)
        cs = []
        if not tail:
            rows = pl.ds(pl.multiple_of(i * ru, 8), ru)
            cs.append(pltpu.make_async_copy(grads[0].at[w, pl.ds(j0, nj), rows, :], g_u.at[k], isem.at[k, 9]))
            cs.append(pltpu.make_async_copy(grads[1].at[w, row, :], g_d.at[k], isem.at[k, 10]))
        for q in range(3):
            for p in range(2):
                cs.append(pltpu.make_async_copy(up_at(states[q], p, i * ru, ru), in_u.at[k, q, p], isem.at[k, 2 * q + p]))
            cs.append(pltpu.make_async_copy(states[3 + q].at[w, row, :], in_d.at[k, q], isem.at[k, 6 + q]))
        return cs

    def stores(i):
        k = lax.rem(i, 2)
        row = pl.ds(pl.multiple_of((i + 2 * j0) * 128, 8), 128)
        cs = []
        for q in range(3):
            for p in range(2):
                cs.append(pltpu.make_async_copy(out_u.at[k, q, p], up_at(outs[q], p, i * ru, ru), osem.at[k, 2 * q + p]))
            cs.append(pltpu.make_async_copy(out_d.at[k, q], outs[3 + q].at[w, row, :], osem.at[k, 6 + q]))
        for p in range(2):
            cs.append(pltpu.make_async_copy(w_u.at[k, p], up_at(outs[6], p, d * (D // 2) + i * ru, ru), osem.at[k, 9 + p]))
        my_down = pl.ds(pl.multiple_of(d * (FF // 2) + (i + 2 * j0) * 128, 8), 128)
        cs.append(pltpu.make_async_copy(w_d.at[k], outs[7].at[w, my_down, :], osem.at[k, 11]))
        cs.append(pltpu.make_async_copy(w_u.at[k], outs[8].at[:, pl.ds(pl.multiple_of(i * ru, 8), ru), :], osem.at[k, 12]))
        cs.append(pltpu.make_async_copy(w_d.at[k], outs[9].at[i], osem.at[k, 13]))
        return cs

    for i in range(NBUF):
        for c in loads(i):
            c.start()
    if tail:
        g_loads = [pltpu.make_async_copy(grads[q], gt.at[q], gsem.at[q]) for q in range(4)]
        for c in g_loads:
            c.start()
        for c in g_loads:
            c.wait()
        r = lax.axis_index('replica')
        x, y = lax.rem(r, 2), lax.div(r, 2)
        a = (1 - d) * x + d * y
        b = (1 - d) * y + d * x

    def block(i, carry):
        k = lax.rem(i, NBUF)
        o = lax.rem(i, 2)
        for c in loads(i):
            c.wait()

        @pl.when(i >= 2)
        def _():
            for c in stores(i - 2):
                c.wait()

        for t in range(ru // 32):
            rows = slice(t * 32, (t + 1) * 32)
            if tail:
                third = i * (ru // 32) + t
                quarter = lax.div(third, 3)
                src = 2 * lax.rem(lax.div(quarter, 2) + a, 2) + lax.rem(lax.rem(quarter, 2) + b, 2)
                g_row = lax.rem(third, 3) * 32
            for p in range(2):
                for j in range(nj):
                    cols = slice(j * HB, (j + 1) * HB)
                    if tail:
                        g = gt[src, j, 1, pl.ds(pl.multiple_of(p * 96 + g_row, 8), 32), :]
                    else:
                        g = g_u[k, j, rows, p * HB:(p + 1) * HB]
                    res = adam_rule(s, g, in_u[k, 0, p, rows, cols], in_u[k, 1, p, rows, cols], in_u[k, 2, p, rows, cols])
                    for q in range(3):
                        out_u[o, q, p, rows, cols] = res[q]
                    w_u[o, p, rows, cols] = res[0].astype(BF16)
        for t in range(8):
            rows = slice(t * 16, (t + 1) * 16)
            if tail:
                half = lax.rem(i, 2)
                src = 2 * lax.rem(half + a, 2) + lax.rem(t // 4 + b, 2)
                g = jnp.concatenate([gt[src, lax.div(i, 2), 0, p * 64 + (t % 4) * 16:p * 64 + (t % 4) * 16 + 16, :] for p in range(3)], axis=1)
            else:
                g = g_d[k, rows, :]
            res = adam_rule(s, g, in_d[k, 0, rows, :], in_d[k, 1, rows, :], in_d[k, 2, rows, :])
            for q in range(3):
                out_d[o, q, rows, :] = res[q]
            w_d[o, rows, :] = res[0].astype(BF16)
        for c in stores(i):
            c.start()

        @pl.when(i + NBUF < n)
        def _():
            for c in loads(i + NBUF):
                c.start()

        return carry

    lax.fori_loop(0, n, block, 0)
    for i in (n - 2, n - 1):
        for c in stores(i):
            c.wait()


def adam(stats, grads, states, prev, w, j0, nj, tail=False):
    any_spec = pl.BlockSpec(memory_space=pl.ANY)
    n = 2 * nj
    ru = D // 2 // n
    full = [jax.ShapeDtypeStruct(v.shape, F32) for v in states]
    whole = [jax.ShapeDtypeStruct((2, D, FF), BF16), jax.ShapeDtypeStruct((2, FF, D), BF16)]
    halves = [jax.ShapeDtypeStruct((2, D // 2, nj * HB), BF16), jax.ShapeDtypeStruct((n, 128, D), BF16)]
    norm = [] if prev else [jax.ShapeDtypeStruct((1,), F32)]
    first = 1 + len(grads) + 6
    cells = D * nj * HB * 2
    vmem, dma = pltpu.VMEM, pltpu.SemaphoreType.DMA
    return pl.pallas_call(
        lambda *refs: adam_kernel(w, j0, nj, tail, len(prev), *refs),
        out_shape=full + whole + halves + norm,
        in_specs=[pl.BlockSpec(memory_space=pltpu.VMEM)] + [any_spec] * (len(grads) + 6 + len(prev)),
        out_specs=[any_spec] * 10 + [pl.BlockSpec(memory_space=pltpu.SMEM)] * len(norm),
        scratch_shapes=[vmem((NBUF, 3, 2, ru, nj * HB), F32), vmem((NBUF, 3, 128, D), F32),
                        vmem((NBUF, nj, ru, BF), F32), vmem((NBUF, 128, D), F32),
                        vmem((2, 3, 2, ru, nj * HB), F32), vmem((2, 3, 128, D), F32),
                        vmem((2, 2, ru, nj * HB), BF16), vmem((2, 128, D), BF16),
                        vmem((4, TAIL, 2, 192, 256), F32), dma((NBUF, 11)), dma((2, 14)), dma((4,))],
        input_output_aliases={first + k: k for k in range(len(prev))},
        compiler_params=pltpu.CompilerParams(vmem_limit_bytes=67043328),
        cost_estimate=pl.CostEstimate(flops=cells * 400, bytes_accessed=cells * 30, transcendentals=0),
    )(stats, *grads, *states, *prev)


def place_kernel(parts, *refs):
    n_in = 2 * len(parts)
    got, (out_u, out_d), refs = refs[:n_in], refs[n_in + 2:n_in + 4], refs[n_in + 4:]
    q = 1 - lax.axis_index('data')
    rows = pl.ds(pl.multiple_of(q * (D // 2), 8), D // 2)
    moves = []
    for k, (w, j0, nj) in enumerate(parts):
        buf_u, buf_d, sem_in, sem_out = refs[4 * k:4 * k + 4]
        for p in range(2):
            moves.append((pltpu.make_async_copy(got[2 * k].at[p], buf_u.at[p], sem_in.at[p]), [
                pltpu.make_async_copy(buf_u.at[p], out_u.at[w, rows, pl.ds((p * NB + j0) * HB, nj * HB)], sem_out.at[p])]))
        for p in range(2):
            part = pl.ds(p * nj, nj)
            stores = []
            for t in range(p * nj, (p + 1) * nj):
                to = pl.ds(pl.multiple_of(q * (FF // 2) + (t + 2 * j0) * 128, 8), 128)
                stores.append(pltpu.make_async_copy(buf_d.at[t], out_d.at[w, to, :], sem_out.at[2 + t]))
            moves.append((pltpu.make_async_copy(got[2 * k + 1].at[part], buf_d.at[part], sem_in.at[2 + p]), stores))
    for load, stores in moves:
        load.start()
    for load, stores in moves:
        load.wait()
        for st in stores:
            st.start()
    for load, stores in moves:
        for st in stores:
            st.wait()


def place(parts, got, weights):
    any_spec = pl.BlockSpec(memory_space=pl.ANY)
    flat = [v for pair in got for v in pair]
    scratch = []
    for w, j0, nj in parts:
        scratch += [pltpu.VMEM((2, D // 2, nj * HB), BF16), pltpu.VMEM((2 * nj, 128, D), BF16),
                    pltpu.SemaphoreType.DMA((4,)), pltpu.SemaphoreType.DMA((2 + 2 * nj,))]
    cells = sum(D * nj * HB * 2 for w, j0, nj in parts)
    return pl.pallas_call(
        lambda *refs: place_kernel(parts, *refs),
        out_shape=(jax.ShapeDtypeStruct((2, D, FF), BF16), jax.ShapeDtypeStruct((2, FF, D), BF16)),
        in_specs=[any_spec] * (len(flat) + 2),
        out_specs=(any_spec, any_spec),
        scratch_shapes=scratch,
        input_output_aliases={len(flat) + k: k for k in range(2)},
        compiler_params=pltpu.CompilerParams(vmem_limit_bytes=67043328),
        cost_estimate=pl.CostEstimate(flops=cells * 100, bytes_accessed=cells * 4, transcendentals=0),
    )(*flat, *weights)


def swap(halves):
    return [lax.ppermute(v, 'data', [(0, 1), (1, 0)]) for v in halves]


def solution(mesh):
    batch_spec = P(('replica', 'data'), None)
    whole_spec = P()
    shard_spec = P(None, 'data', None)
    first_axis = [(r * 2 + d, (r ^ (1 if d == 0 else 2)) * 2 + d) for r in range(4) for d in range(2)]
    second_axis = [(r * 2 + d, (r ^ (2 if d == 0 else 1)) * 2 + d) for r in range(4) for d in range(2)]

    def device_step(inp_rows, out_grad, w_up, w_down, master_up, master_down, mom_up, mom_down, var_up, var_down, clip_norm):
        pre_one, mid_rows = forward(inp_rows, w_up, w_down)
        g_up, g_down, g_tail, stats = backward_reduce(clip_norm.reshape(1), mid_rows, out_grad, inp_rows, pre_one, w_up, w_down)
        axes = ('replica', 'data')
        tails = [g_tail]
        for perm in (second_axis, first_axis):
            tails.append(lax.ppermute(g_tail, axes, perm))
        tails.append(lax.ppermute(tails[1], axes, first_axis))
        states = [master_up, mom_up, var_up, master_down, mom_down, var_down]
        cut = NB - TAIL
        *new, wu, wd, norm = adam(stats, [g_up, g_down], states, [], 1, 0, NB)
        got_a = swap([wu, wd])
        *new, wu, wd = adam(stats, [g_up, g_down], states, new, 0, 0, cut)
        got_b = swap([wu, wd])
        *new, wu, wd = adam(stats, tails, states, new, 0, cut, TAIL, tail=True)
        got_c = swap([wu, wd])
        new[6:] = place([(1, 0, NB), (0, 0, cut)], [got_a, got_b], new[6:])
        new[6:] = place([(0, cut, TAIL)], [got_c], new[6:])
        m_up, o_up, v_up, m_down, o_down, v_down, new_up, new_down = new
        return (new_up, new_down, m_up, m_down, o_up, o_down, v_up, v_down, norm.reshape(()))

    return jax.shard_map(device_step, mesh=mesh, in_specs=(batch_spec, batch_spec, whole_spec, whole_spec, shard_spec, shard_spec, shard_spec, shard_spec, shard_spec, shard_spec, whole_spec), out_specs=(whole_spec, whole_spec, shard_spec, shard_spec, shard_spec, shard_spec, shard_spec, shard_spec, whole_spec), check_vma=False)
```

```python
import jax
import jax.numpy as jnp
from jax import lax
from jax.experimental import pallas as pl
from jax.experimental.pallas import tpu as pltpu
from jax.sharding import PartitionSpec as P


BETA1 = 0.9
BETA2 = 0.95
ADAM_EPS = 1e-8
LEARN_RATE = 5e-3
NORM_EPS = 1e-6
STEP = 10
BIAS_ONE = 1.0 - BETA1 ** STEP
BIAS_TWO = 1.0 - BETA2 ** STEP
MESH = pl.DeviceIdType.MESH
F32 = jnp.float32
BF16 = jnp.bfloat16

B, D, FF = 4096, 768, 3072
HD, HF = D // 2, FF // 2
NN, NT, TN = ((1,), (0,)), ((1,), (1,)), ((0,), (0,))
NB = 6
HB = FF // NB // 2
BF = 2 * HB
R = B // 2
NCH = B // R
STEPS = 2 * NB
SLOTS = 3
TAIL = 3
FULL = STEPS - TAIL
SQRT_HALF = 0.7071067811865476
PDF_SCALE = 0.3989422804014327
NBUF = 4
EXP_SCALE = -0.5 * 1.4426950408889634


def gelu_value(pre_act):
    return pre_act * (0.5 + 0.5 * lax.erf(pre_act * SQRT_HALF))


def dot(a, b, dims):
    return lax.dot_general(a, b, (dims, ((), ())), preferred_element_type=F32)


class Item:
    def __init__(self, rows, cols, refs, sems):
        self.rows, self.cols = rows, cols
        self.acc, self.r0, self.r1, self.r2, self.hh = refs
        self.send, self.recv, self.loc = sems


def mega_kernel(clip_ref, h_hbm, dy_hbm, x_hbm, z_hbm, wu_hbm, wd_hbm,
                gup, gdn, gtail, stats,
                abuf, bbuf, cbuf, wa, wb, zb,
                acc_d, r0_d, r1_d, r2_d, h_d,
                acc_u, r0_u, r1_u, r2_u, h_u,
                ssq, sq_in, asem, bsem, wsem, zsem, tsem, nsend, nrecv,
                send_d, recv_d, loc_d, send_u, recv_u, loc_u):
    r = lax.axis_index('replica')
    d = lax.axis_index('data')
    x = lax.rem(r, 2)
    y = lax.div(r, 2)
    x_off = 1 - 2 * x
    y_off = 2 - 4 * y
    partner = (r, 1 - d)
    n1 = (r + (1 - d) * x_off + d * y_off, d)
    n2 = (r + (1 - d) * y_off + d * x_off, d)
    a = (1 - d) * x + d * y
    b = (1 - d) * y + d * x

    item_d = Item(HB, D, (acc_d, r0_d, r1_d, r2_d, h_d), (send_d, recv_d, loc_d))
    item_u = Item(HD, BF, (acc_u, r0_u, r1_u, r2_u, h_u), (send_u, recv_u, loc_u))

    def rows_of(start, size):
        return pl.ds(pl.multiple_of(start, 8), size)

    def row_copy(src, dst, sem, i):
        rows = rows_of(i * R, R)
        return pltpu.make_async_copy(src.at[rows, :], dst.at[rows, :], sem.at[i])

    def w_copies(s):
        slot = lax.rem(s, 2)
        j = lax.rem(s, NB)
        ph = 1 - lax.div(s, NB)
        up, down = [], []
        for p in range(2):
            cols = pl.ds(pl.multiple_of(p * HF + j * HB, 128), HB)
            up.append(pltpu.make_async_copy(wu_hbm.at[1, :, cols], wa.at[slot, :, p * HB:(p + 1) * HB], wsem.at[slot, p]))
            down.append(pltpu.make_async_copy(wd_hbm.at[ph, cols, :], wb.at[slot, p * HB:(p + 1) * HB, :], wsem.at[slot, 2 + p]))
        return up, down

    def z_copies(s, i):
        j = lax.rem(s, NB)
        out = []
        for p in range(2):
            cols = pl.ds(pl.multiple_of(p * HF + j * HB, 128), HB)
            rows = rows_of(i * R, R)
            out.append(pltpu.make_async_copy(z_hbm.at[rows, cols], zb.at[rows, p * HB:(p + 1) * HB], zsem.at[i, p]))
        return out

    def g_rows(it, s, part, size):
        w = 1 - lax.div(s, NB)
        j = lax.rem(s, NB)
        if it is item_d:
            return gdn.at[w, rows_of(j * HB + part, size), :]
        return gup.at[w, j, rows_of(part, size), :]

    def cp(it, stage, s):
        k = lax.rem(s, SLOTS)
        rows = it.rows
        half, quarter = rows // 2, rows // 4
        if stage == 0:
            src, dst, dev = it.acc.at[rows_of((1 - d) * rows, rows), :], it.r0.at[k], partner
        elif stage == 1:
            src, dst, dev = it.r0.at[k, rows_of((1 - a) * half, half), :], it.r1.at[k], n1
        elif stage == 2:
            src, dst, dev = it.r1.at[k, rows_of((1 - b) * quarter, quarter), :], it.r2.at[k], n2
        elif stage == 3:
            q = rows_of(b * quarter, quarter)
            src, dst, dev = it.hh.at[k, q, :], it.hh.at[k, q, :], n2
        else:
            src, dst, dev = it.hh.at[k], g_rows(it, s, a * half, half), n1
        return pltpu.make_async_remote_copy(src_ref=src, dst_ref=dst, send_sem=it.send.at[stage, k],
                                            recv_sem=it.recv.at[stage, k], device_id=dev, device_id_type=MESH)

    def local_out(it, s):
        k = lax.rem(s, SLOTS)
        half = it.rows // 2
        return pltpu.make_async_copy(it.hh.at[k], g_rows(it, s, a * half, half), it.loc.at[k])

    def fold(it, stage, s):
        k = lax.rem(s, SLOTS)
        rows = it.rows
        half, quarter = rows // 2, rows // 4
        if stage == 0:
            return
        cp(it, stage - 1, s).wait()
        if stage == 1:
            it.r0[k] = it.r0[k] + it.acc[rows_of(d * rows, rows), :]
        elif stage == 2:
            it.r1[k] = it.r1[k] + it.r0[k, rows_of(a * half, half), :]
        elif stage == 3:
            g = (it.r2[k] + it.r1[k, rows_of(b * quarter, quarter), :]) * 0.125
            it.hh[k, rows_of(b * quarter, quarter), :] = g
            sq = g * g
            sq = sq.reshape(quarter // 8, 8, it.cols).sum(axis=0)
            tot = sq[:, :128]
            for c in range(1, it.cols // 128):
                tot = tot + sq[:, c * 128:(c + 1) * 128]
            ssq[0] += tot
        elif stage == 5:
            local_out(it, s).wait()

    def tail_out(it, s):
        k = lax.rem(s, SLOTS)
        quarter = it.rows // 4
        ty = 0 if it is item_d else 1
        return [pltpu.make_async_copy(it.hh.at[k, rows_of(b * quarter, quarter), p * 256:(p + 1) * 256],
                                      gtail.at[s - FULL, ty, p * quarter:(p + 1) * quarter, :],
                                      tsem.at[s - FULL, ty, p]) for p in range(it.cols // 256)]

    def post(it, stage, s):
        if stage == 3:
            @pl.when(s < FULL)
            def _():
                cp(it, 3, s).start()

            @pl.when(s >= FULL)
            def _():
                for c in tail_out(it, s):
                    c.start()
        elif stage < 5:
            cp(it, stage, s).start()
        if stage == 4:
            local_out(it, s).start()

    def tick(s, plan):
        late = None
        for it, stage, lag in plan:
            t = s - lag
            ok = jnp.logical_and(t >= 0, t < (FULL if stage >= 4 else STEPS))

            @pl.when(ok)
            def _():
                fold(it, stage, t)

            if late is not None:
                pit, pstage, pt, pok = late

                @pl.when(pok)
                def _():
                    post(pit, pstage, pt)
            late = (it, stage, t, ok)
        pit, pstage, pt, pok = late

        @pl.when(pok)
        def _():
            post(pit, pstage, pt)

    ssq[0] = jnp.zeros((8, 128), F32)
    up, down = w_copies(0)
    for c in [row_copy(h_hbm, abuf, asem, 0)] + up + [row_copy(dy_hbm, bbuf, bsem, 0)] + down:
        c.start()

    barrier = pltpu.get_barrier_semaphore()
    peers = [(2 * (y + fy - 2 * fy * y) + x + fx - 2 * fx * x, d + fd - 2 * fd * d)
             for fy in range(2) for fx in range(2) for fd in range(2)]
    for dev in peers[1:]:
        pl.semaphore_signal(barrier, inc=1, device_id=dev, device_id_type=MESH)
    pl.semaphore_wait(barrier, 7)

    def zero_c(i, carry):
        cbuf[rows_of(i * 128, 128), :] = jnp.zeros((128, D), F32)
        return carry

    lax.fori_loop(0, B // 128, zero_c, 0)

    def gelu_dot(zf, rows, i):
        u = (zf * (0.5 + 0.5 * lax.erf(zf * SQRT_HALF))).astype(BF16)
        acc_d[...] = jnp.where(i == 0, 0.0, acc_d[...]) + dot(u, bbuf[rows, :], TN)

    def pass_one(s, i):
        slot = lax.rem(s, 2)
        rows = rows_of(i * R, R)

        @pl.when(s < NB)
        def _():
            @pl.when(s == 0)
            def _():
                row_copy(h_hbm, abuf, asem, i).wait()
                row_copy(dy_hbm, bbuf, bsem, i).wait()

                @pl.when(i + 1 < NCH)
                def _():
                    row_copy(h_hbm, abuf, asem, i + 1).start()
                    row_copy(dy_hbm, bbuf, bsem, i + 1).start()

            z = dot(abuf[rows, :], wa[slot], NN).astype(BF16)
            zb[rows, :] = z
            gelu_dot(z.astype(F32), rows, i)

        @pl.when(s >= NB)
        def _():
            for c in z_copies(s, i):
                c.wait()
            gelu_dot(zb[rows, :].astype(F32), rows, i)

    def slope_dot(s, rows, i):
        slot = lax.rem(s, 2)
        e = dot(bbuf[rows, :], wb[slot], NT).astype(BF16)
        zf = zb[rows, :].astype(F32)
        slope = 0.5 + 0.5 * lax.erf(zf * SQRT_HALF) + zf * jnp.exp2(zf * zf * EXP_SCALE) * PDF_SCALE
        dd = (e.astype(F32) * slope).astype(BF16)
        acc_u[...] = jnp.where(i == 0, 0.0, acc_u[...]) + dot(abuf[rows, :], dd, TN)
        return dd

    def pass_two(s, i):
        slot = lax.rem(s, 2)
        rows = rows_of(i * R, R)

        @pl.when(s < NB)
        def _():
            dd = slope_dot(s, rows, i)
            cbuf[rows, :] += dot(dd, wa[slot], NT)

        @pl.when(s >= NB)
        def _():
            @pl.when(s == NB)
            def _():
                row_copy(x_hbm, abuf, asem, i).wait()

            slope_dot(s, rows, i)

        @pl.when(jnp.logical_and(s + 1 >= NB, s + 1 < STEPS))
        def _():
            for c in z_copies(s + 1, i):
                c.start()

    plans = (((item_u, 1, 1), (item_d, 4, 2)),
             ((item_d, 2, 1), (item_u, 3, 2), (item_d, 0, 0)),
             ((item_d, 1, 0), (item_d, 3, 1), (item_u, 5, 3)),
             ((item_u, 2, 1), (item_u, 4, 2), (item_d, 5, 2), (item_u, 0, 0)))

    def quarter(t, carry):
        s = lax.div(t, 4)
        pos = lax.rem(t, 4)
        i = lax.rem(pos, 2)

        @pl.when(t == 4 * NB)
        def _():
            for k in range(NCH):
                row_copy(x_hbm, abuf, asem, k).start()

            def conv(k, carry):
                rows = rows_of(k * 128, 128)
                bbuf[rows, :] = cbuf[rows, :].astype(BF16)
                return carry

            lax.fori_loop(0, B // 128, conv, 0)

        @pl.when(jnp.logical_and(pos == 0, s < STEPS))
        def _():
            up, down = w_copies(s)
            for c in down:
                c.wait()

            @pl.when(s < NB)
            def _():
                for c in up:
                    c.wait()

            @pl.when(s + 1 < STEPS)
            def _():
                up, down = w_copies(s + 1)
                for c in down:
                    c.start()

                @pl.when(s + 1 < NB)
                def _():
                    for c in up:
                        c.start()

        @pl.when(jnp.logical_and(pos < 2, s < STEPS))
        def _():
            pass_one(s, i)

        @pl.when(jnp.logical_and(pos >= 2, s < STEPS))
        def _():
            pass_two(s, i)

        for k, plan in enumerate(plans):
            @pl.when(pos == k)
            def _():
                tick(s, plan)
        return carry

    lax.fori_loop(0, 4 * (STEPS + 1) + 2, quarter, 0)

    sq_in[0] = ssq[0]
    for t in range(FULL, STEPS):
        for it in (item_d, item_u):
            for tc in tail_out(it, t):
                tc.wait()
    exchange = [pltpu.make_async_remote_copy(src_ref=ssq.at[0], dst_ref=sq_in.at[k], send_sem=nsend.at[k],
                                             recv_sem=nrecv.at[k], device_id=peers[k], device_id_type=MESH)
                for k in range(1, 8)]
    for c in exchange:
        c.start()
    for c in exchange:
        c.wait()
    total = jnp.zeros((8, 128), F32)
    for iy in range(2):
        for ix in range(2):
            for dd in range(2):
                total = total + sq_in[4 * lax.rem(iy + y, 2) + 2 * lax.rem(ix + x, 2) + lax.rem(dd + d, 2)]
    total = jnp.sum(total, axis=0, keepdims=True)
    total = jnp.sum(total, axis=1, keepdims=True)
    norm = jnp.sqrt(total)
    scale = jnp.minimum(1.0, clip_ref[0] / (norm + NORM_EPS))
    stats[0] = jnp.broadcast_to(norm, (8, 128))
    stats[1] = jnp.broadcast_to(scale, (8, 128))


def backward_reduce(clip, h, dy, x, z1, w_up, w_down):
    any_spec = pl.BlockSpec(memory_space=pl.ANY)
    vmem = pltpu.VMEM

    def item(rows, cols, acc):
        return [vmem(acc, F32), vmem((SLOTS, rows, cols), F32), vmem((SLOTS, rows // 2, cols), F32),
                vmem((SLOTS, rows // 4, cols), F32), vmem((SLOTS, rows // 2, cols), F32)]

    dma = pltpu.SemaphoreType.DMA
    return pl.pallas_call(
        mega_kernel,
        out_shape=(jax.ShapeDtypeStruct((2, NB, HD, BF), F32),
                   jax.ShapeDtypeStruct((2, HF, D), F32),
                   jax.ShapeDtypeStruct((TAIL, 2, 192, 256), F32),
                   jax.ShapeDtypeStruct((2, 8, 128), F32)),
        in_specs=[pl.BlockSpec(memory_space=pltpu.SMEM)] + [any_spec] * 6,
        out_specs=(any_spec, any_spec, any_spec, pl.BlockSpec(memory_space=pltpu.VMEM)),
        scratch_shapes=[vmem((B, D), BF16), vmem((B, D), BF16), vmem((B, D), F32),
                        vmem((2, D, BF), BF16), vmem((2, BF, D), BF16), vmem((B, BF), BF16)]
        + item(HB, D, (BF, D)) + item(HD, BF, (D, BF))
        + [vmem((1, 8, 128), F32), vmem((8, 8, 128), F32)]
        + [dma((NCH,)), dma((NCH,)), dma((2, 4)), dma((NCH, 2)), dma((TAIL, 2, 3)), dma((8,)), dma((8,))]
        + [dma((5, SLOTS)), dma((5, SLOTS)), dma((SLOTS,))] * 2,
        compiler_params=pltpu.CompilerParams(collective_id=0, has_side_effects=True, vmem_limit_bytes=67043328),
        name='backward_reduce',
    )(clip, h, dy, x, z1, w_up, w_down)


def forward_body(x, wu, wd, z_ref, h_ref):
    z = dot(x[...], wu[0], NN).astype(BF16)
    z_ref[...] = z
    u = gelu_value(z.astype(F32)).astype(BF16)
    h_ref[...] = dot(u, wd[0], NN).astype(BF16)


def forward(x, w_up, w_down):
    rows = 1024
    once = pl.Buffered(1)
    return pl.pallas_call(
        forward_body,
        grid=(B // rows,),
        out_shape=(jax.ShapeDtypeStruct((B, FF), BF16), jax.ShapeDtypeStruct((B, D), BF16)),
        in_specs=[pl.BlockSpec((rows, D), lambda i: (i, 0)),
                  pl.BlockSpec((1, D, FF), lambda i: (0, 0, 0), pipeline_mode=once),
                  pl.BlockSpec((1, FF, D), lambda i: (0, 0, 0), pipeline_mode=once)],
        out_specs=(pl.BlockSpec((rows, FF), lambda i: (i, 0)), pl.BlockSpec((rows, D), lambda i: (i, 0))),
        compiler_params=pltpu.CompilerParams(vmem_limit_bytes=67043328),
        name='forward',
    )(x, w_up, w_down)


def adam_rule(s, g, master, mom, var):
    mom = BETA1 * mom + (1.0 - BETA1) * s * g
    var = BETA2 * var + (1.0 - BETA2) * (s * s) * (g * g)
    master = master - LEARN_RATE * (mom / BIAS_ONE) / (jnp.sqrt(var / BIAS_TWO) + ADAM_EPS)
    return master, mom, var


def adam_kernel(w, j0, nj, tail, n_alias, stats, *refs):
    n = 2 * nj
    ru = HD // n
    n_grads = 4 if tail else 2
    grads, refs = refs[:n_grads], refs[n_grads:]
    states, refs = refs[:6], refs[6 + n_alias:]
    outs, refs = refs[:10], refs[10:]
    if not n_alias:
        norm_out, refs = refs[0], refs[1:]
        norm_out[0] = jnp.max(stats[0])
    in_u, in_d, g_u, g_d, out_u, out_d, w_u, w_d, gt, isem, osem, gsem = refs
    d = lax.axis_index('data')
    s = stats[1, 0:1, 0:1]

    def up_at(ref, p, row0, size):
        return ref.at[w, pl.ds(pl.multiple_of(row0, 8), size), pl.ds((p * NB + j0) * HB, nj * HB)]

    def loads(i):
        k = lax.rem(i, NBUF)
        row = pl.ds(pl.multiple_of((i + 2 * j0) * 128, 8), 128)
        cs = []
        if not tail:
            rows = pl.ds(pl.multiple_of(i * ru, 8), ru)
            cs.append(pltpu.make_async_copy(grads[0].at[w, pl.ds(j0, nj), rows, :], g_u.at[k], isem.at[k, 9]))
            cs.append(pltpu.make_async_copy(grads[1].at[w, row, :], g_d.at[k], isem.at[k, 10]))
        for q in range(3):
            for p in range(2):
                cs.append(pltpu.make_async_copy(up_at(states[q], p, i * ru, ru), in_u.at[k, q, p], isem.at[k, 2 * q + p]))
            cs.append(pltpu.make_async_copy(states[3 + q].at[w, row, :], in_d.at[k, q], isem.at[k, 6 + q]))
        return cs

    def stores(i):
        k = lax.rem(i, 2)
        row = pl.ds(pl.multiple_of((i + 2 * j0) * 128, 8), 128)
        cs = []
        for q in range(3):
            for p in range(2):
                cs.append(pltpu.make_async_copy(out_u.at[k, q, p], up_at(outs[q], p, i * ru, ru), osem.at[k, 2 * q + p]))
            cs.append(pltpu.make_async_copy(out_d.at[k, q], outs[3 + q].at[w, row, :], osem.at[k, 6 + q]))
        for p in range(2):
            cs.append(pltpu.make_async_copy(w_u.at[k, p], up_at(outs[6], p, d * HD + i * ru, ru), osem.at[k, 9 + p]))
        my_down = pl.ds(pl.multiple_of(d * HF + (i + 2 * j0) * 128, 8), 128)
        cs.append(pltpu.make_async_copy(w_d.at[k], outs[7].at[w, my_down, :], osem.at[k, 11]))
        cs.append(pltpu.make_async_copy(w_u.at[k], outs[8].at[:, pl.ds(pl.multiple_of(i * ru, 8), ru), :], osem.at[k, 12]))
        cs.append(pltpu.make_async_copy(w_d.at[k], outs[9].at[i], osem.at[k, 13]))
        return cs

    for i in range(NBUF):
        for c in loads(i):
            c.start()
    if tail:
        g_loads = [pltpu.make_async_copy(grads[q], gt.at[q], gsem.at[q]) for q in range(4)]
        for c in g_loads:
            c.start()
        for c in g_loads:
            c.wait()
        r = lax.axis_index('replica')
        x, y = lax.rem(r, 2), lax.div(r, 2)
        a = (1 - d) * x + d * y
        b = (1 - d) * y + d * x

    def block(i, carry):
        k = lax.rem(i, NBUF)
        o = lax.rem(i, 2)
        for c in loads(i):
            c.wait()

        @pl.when(i >= 2)
        def _():
            for c in stores(i - 2):
                c.wait()

        for t in range(ru // 32):
            rows = slice(t * 32, (t + 1) * 32)
            if tail:
                third = i * (ru // 32) + t
                quarter = lax.div(third, 3)
                src = 2 * lax.rem(lax.div(quarter, 2) + a, 2) + lax.rem(lax.rem(quarter, 2) + b, 2)
                g_row = lax.rem(third, 3) * 32
            for p in range(2):
                for j in range(nj):
                    cols = slice(j * HB, (j + 1) * HB)
                    if tail:
                        g = gt[src, j, 1, pl.ds(pl.multiple_of(p * 96 + g_row, 8), 32), :]
                    else:
                        g = g_u[k, j, rows, p * HB:(p + 1) * HB]
                    res = adam_rule(s, g, in_u[k, 0, p, rows, cols], in_u[k, 1, p, rows, cols], in_u[k, 2, p, rows, cols])
                    for q in range(3):
                        out_u[o, q, p, rows, cols] = res[q]
                    w_u[o, p, rows, cols] = res[0].astype(BF16)
        for t in range(8):
            rows = slice(t * 16, (t + 1) * 16)
            if tail:
                half = lax.rem(i, 2)
                src = 2 * lax.rem(half + a, 2) + lax.rem(t // 4 + b, 2)
                g = jnp.concatenate([gt[src, lax.div(i, 2), 0, p * 64 + (t % 4) * 16:p * 64 + (t % 4) * 16 + 16, :] for p in range(3)], axis=1)
            else:
                g = g_d[k, rows, :]
            res = adam_rule(s, g, in_d[k, 0, rows, :], in_d[k, 1, rows, :], in_d[k, 2, rows, :])
            for q in range(3):
                out_d[o, q, rows, :] = res[q]
            w_d[o, rows, :] = res[0].astype(BF16)
        for c in stores(i):
            c.start()

        @pl.when(i + NBUF < n)
        def _():
            for c in loads(i + NBUF):
                c.start()

        return carry

    lax.fori_loop(0, n, block, 0)
    for i in (n - 2, n - 1):
        for c in stores(i):
            c.wait()


def adam(stats, grads, states, prev, w, j0, nj, tail=False):
    any_spec = pl.BlockSpec(memory_space=pl.ANY)
    n = 2 * nj
    ru = HD // n
    full = [jax.ShapeDtypeStruct(v.shape, F32) for v in states]
    whole = [jax.ShapeDtypeStruct((2, D, FF), BF16), jax.ShapeDtypeStruct((2, FF, D), BF16)]
    halves = [jax.ShapeDtypeStruct((2, HD, nj * HB), BF16), jax.ShapeDtypeStruct((n, 128, D), BF16)]
    norm = [] if prev else [jax.ShapeDtypeStruct((1,), F32)]
    first = 1 + len(grads) + 6
    cells = D * nj * HB * 2
    vmem, dma = pltpu.VMEM, pltpu.SemaphoreType.DMA
    return pl.pallas_call(
        lambda *refs: adam_kernel(w, j0, nj, tail, len(prev), *refs),
        out_shape=full + whole + halves + norm,
        in_specs=[pl.BlockSpec(memory_space=pltpu.VMEM)] + [any_spec] * (len(grads) + 6 + len(prev)),
        out_specs=[any_spec] * 10 + [pl.BlockSpec(memory_space=pltpu.SMEM)] * len(norm),
        scratch_shapes=[vmem((NBUF, 3, 2, ru, nj * HB), F32), vmem((NBUF, 3, 128, D), F32),
                        vmem((NBUF, nj, ru, BF), F32), vmem((NBUF, 128, D), F32),
                        vmem((2, 3, 2, ru, nj * HB), F32), vmem((2, 3, 128, D), F32),
                        vmem((2, 2, ru, nj * HB), BF16), vmem((2, 128, D), BF16),
                        vmem((4, TAIL, 2, 192, 256), F32), dma((NBUF, 11)), dma((2, 14)), dma((4,))],
        input_output_aliases={first + k: k for k in range(len(prev))},
        compiler_params=pltpu.CompilerParams(vmem_limit_bytes=67043328),
        cost_estimate=pl.CostEstimate(flops=cells * 400, bytes_accessed=cells * 30, transcendentals=0),
    )(stats, *grads, *states, *prev)


def place_kernel(parts, *refs):
    n_in = 2 * len(parts)
    got, (out_u, out_d), refs = refs[:n_in], refs[n_in + 2:n_in + 4], refs[n_in + 4:]
    q = 1 - lax.axis_index('data')
    rows = pl.ds(pl.multiple_of(q * HD, 8), HD)
    moves = []
    for k, (w, j0, nj) in enumerate(parts):
        buf_u, buf_d, sem_in, sem_out = refs[4 * k:4 * k + 4]
        for p in range(2):
            moves.append((pltpu.make_async_copy(got[2 * k].at[p], buf_u.at[p], sem_in.at[p]), [
                pltpu.make_async_copy(buf_u.at[p], out_u.at[w, rows, pl.ds((p * NB + j0) * HB, nj * HB)], sem_out.at[p])]))
        for p in range(2):
            part = pl.ds(p * nj, nj)
            stores = []
            for t in range(p * nj, (p + 1) * nj):
                to = pl.ds(pl.multiple_of(q * HF + (t + 2 * j0) * 128, 8), 128)
                stores.append(pltpu.make_async_copy(buf_d.at[t], out_d.at[w, to, :], sem_out.at[2 + t]))
            moves.append((pltpu.make_async_copy(got[2 * k + 1].at[part], buf_d.at[part], sem_in.at[2 + p]), stores))
    for load, stores in moves:
        load.start()
    for load, stores in moves:
        load.wait()
        for st in stores:
            st.start()
    for load, stores in moves:
        for st in stores:
            st.wait()


def place(parts, got, weights):
    any_spec = pl.BlockSpec(memory_space=pl.ANY)
    flat = [v for pair in got for v in pair]
    scratch = []
    for w, j0, nj in parts:
        scratch += [pltpu.VMEM((2, HD, nj * HB), BF16), pltpu.VMEM((2 * nj, 128, D), BF16),
                    pltpu.SemaphoreType.DMA((4,)), pltpu.SemaphoreType.DMA((2 + 2 * nj,))]
    cells = sum(D * nj * HB * 2 for w, j0, nj in parts)
    return pl.pallas_call(
        lambda *refs: place_kernel(parts, *refs),
        out_shape=(jax.ShapeDtypeStruct((2, D, FF), BF16), jax.ShapeDtypeStruct((2, FF, D), BF16)),
        in_specs=[any_spec] * (len(flat) + 2),
        out_specs=(any_spec, any_spec),
        scratch_shapes=scratch,
        input_output_aliases={len(flat) + k: k for k in range(2)},
        compiler_params=pltpu.CompilerParams(vmem_limit_bytes=67043328),
        cost_estimate=pl.CostEstimate(flops=cells * 100, bytes_accessed=cells * 4, transcendentals=0),
    )(*flat, *weights)


def swap(halves):
    return [lax.ppermute(v, 'data', [(0, 1), (1, 0)]) for v in halves]


def solution(mesh):
    batch_spec = P(('replica', 'data'), None)
    whole_spec = P()
    shard_spec = P(None, 'data', None)
    first_axis = [(r * 2 + d, (r ^ (1 if d == 0 else 2)) * 2 + d) for r in range(4) for d in range(2)]
    second_axis = [(r * 2 + d, (r ^ (2 if d == 0 else 1)) * 2 + d) for r in range(4) for d in range(2)]

    def device_step(inp_rows, out_grad, w_up, w_down, master_up, master_down, mom_up, mom_down, var_up, var_down, clip_norm):
        pre_one, mid_rows = forward(inp_rows, w_up, w_down)
        g_up, g_down, g_tail, stats = backward_reduce(clip_norm.reshape(1), mid_rows, out_grad, inp_rows, pre_one, w_up, w_down)
        axes = ('replica', 'data')
        tails = [g_tail]
        for perm in (second_axis, first_axis):
            tails.append(lax.ppermute(g_tail, axes, perm))
        tails.append(lax.ppermute(tails[1], axes, first_axis))
        states = [master_up, mom_up, var_up, master_down, mom_down, var_down]
        cut = NB - TAIL
        *new, wu, wd, norm = adam(stats, [g_up, g_down], states, [], 1, 0, NB)
        got_a = swap([wu, wd])
        *new, wu, wd = adam(stats, [g_up, g_down], states, new, 0, 0, cut)
        got_b = swap([wu, wd])
        *new, wu, wd = adam(stats, tails, states, new, 0, cut, TAIL, tail=True)
        got_c = swap([wu, wd])
        new[6:] = place([(1, 0, NB), (0, 0, cut)], [got_a, got_b], new[6:])
        new[6:] = place([(0, cut, TAIL)], [got_c], new[6:])
        m_up, o_up, v_up, m_down, o_down, v_down, new_up, new_down = new
        return (new_up, new_down, m_up, m_down, o_up, o_down, v_up, v_down, norm.reshape(()))

    return jax.shard_map(device_step, mesh=mesh, in_specs=(batch_spec, batch_spec, whole_spec, whole_spec, shard_spec, shard_spec, shard_spec, shard_spec, shard_spec, shard_spec, whole_spec), out_specs=(whole_spec, whole_spec, shard_spec, shard_spec, shard_spec, shard_spec, shard_spec, shard_spec, whole_spec), check_vma=False)
```
